32 devices in a mesh: dp: 8 (over z, y), seq: 4 (over x, core).
Axes of the slice: x: 2, y: 2, z: 4, core: 2. Of those that a mesh axis runs over, the one named last changes fastest.
Arguments:
- layer_input: bfloat16 [8, 512, 2048], P('dp', 'seq'), may hold values from -6 to 6
- writes_first: bfloat16 [8, 512, 128], P('dp', 'seq'), may hold values from -0.375 to 0.375
- reads_first: bfloat16 [8, 512, 128], P('dp', 'seq'), may hold values from -0.375 to 0.375
- decay_first: float32 [8, 32, 512], P('dp', None, 'seq'), may hold values from -1.5 to 0, as said below
- skip_first: float32 [32], replicated, may hold values from 0.5 to 1.5
- writes_second: bfloat16 [8, 512, 128], P('dp', 'seq'), may hold values from -0.375 to 0.375
- reads_second: bfloat16 [8, 512, 128], P('dp', 'seq'), may hold values from -0.375 to 0.375
- decay_second: float32 [8, 32, 512], P('dp', None, 'seq'), may hold values from -1.5 to 0, as said below
- skip_second: float32 [32], replicated, may hold values from 0.5 to 1.5
- order_first: int32 [512], P('seq'), may hold values from 0 to 511, as said below
- order_second: int32 [512], P('seq'), may hold values from 0 to 511, as said below
- cotangent: float32 [8, 512, 2048], P('dp', 'seq'), may hold values from -48 to 48
Outputs:
- grad_input: bfloat16 [8, 512, 2048], P('dp', 'seq')
- grad_writes_first: bfloat16 [8, 512, 128], P('dp', 'seq')
- grad_reads_first: bfloat16 [8, 512, 128], P('dp', 'seq')
- grad_decay_first: float32 [8, 32, 512], P('dp', None, 'seq')
- grad_skip_first: float32 [32], replicated
- grad_writes_second: bfloat16 [8, 512, 128], P('dp', 'seq')
- grad_reads_second: bfloat16 [8, 512, 128], P('dp', 'seq')
- grad_decay_second: float32 [8, 32, 512], P('dp', None, 'seq')
- grad_skip_second: float32 [32], replicated
The draws below stay inside these ranges and needn't reach their ends.
Inputs may be any that keep to these rules, and one draw needn't show every extreme that they name: order_first lists the cells of a 16 by 32 grid (cell i * 32 + j for row i, column j) row after row from row 0 on, each row left to right or right to left. order_second lists the same cells column after column from column 0 on, each column top to bottom or bottom to top. `decay_first`: every entry is negative. `decay_second`: every entry is negative.
All inputs are finite; a program needn't handle non-finite values.
Results may differ from the reference program's by a relative error of at most 0.005.
Values may be sent and summed in bfloat16 or wider, within the bound.
A program may use at most 128 MiB of HBM per device.

```python
import math
import jax
import jax.numpy as jnp
from jax import lax

HEADS = 32
HEAD_DIM = 64
STATE = 128
GROUP = 128
COLS = 32
WIDTH = 2048
ROWS = 16
CLIP_TOKENS = 512
CLIP_COUNT = 8


def decay_law(key):
    random_key_sequence = jax.random.split(key, 6)
    fast_share = 0.5
    is_fast = jax.random.uniform(random_key_sequence[0], (HEADS,)) < fast_share
    fast_rate = jnp.exp(jax.random.uniform(random_key_sequence[1], (HEADS,), minval=jnp.log(1.0 / 50.0), maxval=jnp.log(1.0 / 30.0)))
    slow_rate = jnp.exp(jax.random.uniform(random_key_sequence[2], (HEADS,), minval=jnp.log(0.05), maxval=jnp.log(0.35))) / CLIP_TOKENS
    base_rate = jnp.where(is_fast, fast_rate, slow_rate)
    roughness = jax.random.uniform(random_key_sequence[3], (CLIP_COUNT, HEADS, CLIP_TOKENS), minval=0.5, maxval=1.5)
    block_scale = jnp.exp(jax.random.uniform(random_key_sequence[4], (CLIP_COUNT, 1, CLIP_TOKENS // GROUP), minval=jnp.log(0.6), maxval=jnp.log(1.6)))
    block_scale = jnp.repeat(block_scale, GROUP, axis=2)
    decay_rate_every = base_rate[None, :, None] * roughness * block_scale
    spike_random_keys = jax.random.split(random_key_sequence[5], 2)
    spike_location = jax.random.randint(spike_random_keys[0], (CLIP_COUNT, 2), 0, CLIP_TOKENS)
    spike_penalty_loss = jax.random.uniform(spike_random_keys[1], (CLIP_COUNT, 2), minval=0.2, maxval=0.5)
    token_position = jnp.arange(CLIP_TOKENS, dtype=jnp.int32)
    spike_penalty_terms = (token_position[None, None, :] == spike_location[:, :, None]).astype(jnp.float32) * jnp.log(1.0 - spike_penalty_loss)[:, :, None]
    return (jnp.sum(spike_penalty_terms, axis=1)[:, None, :] - decay_rate_every).astype(jnp.float32)


def draw_decay_first(key, part):
    return decay_law(jax.random.fold_in(key, 11))


def draw_decay_second(key, part):
    return decay_law(jax.random.fold_in(key, 12))


def draw_order_first(key, part):
    reversed_rows = jax.random.randint(jax.random.fold_in(key, 21), (ROWS,), 0, 2)
    token_position = jnp.arange(CLIP_TOKENS, dtype=jnp.int32)
    row_ids = token_position // COLS
    col_ids = token_position % COLS
    return (row_ids * COLS + jnp.where(reversed_rows[row_ids] == 1, COLS - 1 - col_ids, col_ids)).astype(jnp.int32)


def draw_order_second(key, part):
    reversed_cols = jax.random.randint(jax.random.fold_in(key, 22), (COLS,), 0, 2)
    token_position = jnp.arange(CLIP_TOKENS, dtype=jnp.int32)
    col_ids = token_position // ROWS
    row_ids = token_position % ROWS
    return (jnp.where(reversed_cols[col_ids] == 1, ROWS - 1 - row_ids, row_ids) * COLS + col_ids).astype(jnp.int32)


def draw_cotangent(key, part):
    key_one = jax.random.fold_in(key, 31)
    clip_rise = 3.0 ** (jnp.arange(CLIP_COUNT, dtype=jnp.float32) / CLIP_COUNT)
    token_position = jnp.arange(CLIP_TOKENS, dtype=jnp.float32) / CLIP_TOKENS
    noise_all = jnp.clip(jax.random.normal(key_one, (CLIP_COUNT, CLIP_TOKENS, HEADS * HEAD_DIM)), -5.0, 5.0)
    seq_rise = 3.0 ** token_position
    return (noise_all * clip_rise[:, None, None] * seq_rise[None, :, None]).astype(jnp.float32)


def steps_of(own_key, shape, cuts, least, high):
    gain = 1.0
    for dim, shards_of in cuts:
        draws = jax.random.uniform(jax.random.fold_in(jax.random.fold_in(own_key, 6), dim), (shards_of,), jnp.float32, least / len(cuts), high / len(cuts))
        gain = gain * jnp.repeat(jnp.exp(draws), shape[dim] // shards_of).reshape((-1,) + (1,) * (len(shape) - 1 - dim))
    return gain


def noise(rng, dims, deviation, bound, shards=(), kind=jnp.bfloat16):
    drawn = jax.random.normal(rng, dims, jnp.float32) * deviation
    if len(shards) > 0:
        drawn = steps_of(rng, dims, shards, -0.22, 0.18) * drawn
    return jnp.clip(drawn, min=-bound, max=bound).astype(kind)


def setup_inputs(seed: int = 0) -> dict:
    keys = jax.random.split(jax.random.key(seed), 13)
    return {
        "layer_input": noise(keys[0], (CLIP_COUNT, CLIP_TOKENS, WIDTH), 1.0, 6.0, ((0, 8), (1, 4))),
        "writes_first": noise(keys[1], (CLIP_COUNT, CLIP_TOKENS, STATE), ((CLIP_TOKENS * STATE) ** -0.25), 0.375, ((0, 8), (1, 4))),
        "reads_first": noise(keys[2], (CLIP_COUNT, CLIP_TOKENS, STATE), ((CLIP_TOKENS * STATE) ** -0.25), 0.375, ((0, 8), (1, 4))),
        "decay_first": draw_decay_first(jax.random.fold_in(keys[12], 71), 0),
        "skip_first": jnp.clip(jax.random.uniform(keys[4], (HEADS,), jnp.float32, 0.5, 1.5), 0.5, 1.5),
        "writes_second": noise(keys[5], (CLIP_COUNT, CLIP_TOKENS, STATE), ((CLIP_TOKENS * STATE) ** -0.25), 0.375, ((0, 8), (1, 4))),
        "reads_second": noise(keys[6], (CLIP_COUNT, CLIP_TOKENS, STATE), ((CLIP_TOKENS * STATE) ** -0.25), 0.375, ((0, 8), (1, 4))),
        "decay_second": draw_decay_second(jax.random.fold_in(keys[12], 71), 0),
        "skip_second": jnp.clip(jax.random.uniform(keys[8], (HEADS,), jnp.float32, 0.5, 1.5), 0.5, 1.5),
        "order_first": draw_order_first(jax.random.fold_in(keys[12], 71), 0),
        "order_second": draw_order_second(jax.random.fold_in(keys[12], 71), 0),
        "cotangent": draw_cotangent(jax.random.fold_in(keys[12], 71), 0),
    }


highest = lax.Precision.HIGHEST

def group_step(carried, pieces, skip):
    inputs, writes, reads, log_decay = pieces
    running = jnp.cumsum(log_decay, axis=0)
    length = inputs.shape[0]
    causal = jnp.tril(jnp.ones((length, length), dtype=bool))
    scores = jnp.dot(reads, writes.T, precision=highest)
    log_gap = running.T[:, :, None] - running.T[:, None, :]
    weights = jnp.where(causal[None], jnp.exp(jnp.where(causal[None], log_gap, 0.0)), 0.0) * scores[None]
    outputs = jnp.einsum('hts,shp->thp', weights, inputs, precision=highest)
    carried_out = jnp.einsum('hpn,tn->thp', carried, reads, precision=highest)
    outputs = outputs + jnp.exp(running)[:, :, None] * carried_out + skip[None, :, None] * inputs
    totals = running[-1]
    scaled = inputs * jnp.exp(totals[None, :] - running)[:, :, None]
    carried = jnp.exp(totals)[:, None, None] * carried + jnp.einsum('shp,sn->hpn', scaled, writes, precision=highest)
    return (carried, outputs)

def run_layer(inputs, writes, reads, log_decay, skip, carried):
    length, features = inputs.shape
    head_count = log_decay.shape[1]
    head_size = features // head_count
    block_count = length // GROUP
    stacked = (inputs.reshape(block_count, GROUP, head_count, head_size), writes.reshape(block_count, GROUP, writes.shape[1]), reads.reshape(block_count, GROUP, reads.shape[1]), log_decay.reshape(block_count, GROUP, head_count))
    carried, outputs = lax.scan(lambda carry_now, pieces: group_step(carry_now, pieces, skip), carried, stacked)
    return (outputs.reshape(length, features), carried)

def reference(layer_input, writes_first, reads_first, decay_first, skip_first, writes_second, reads_second, decay_second, skip_second, order_first, order_second, cotangent):
    features = HEADS * HEAD_DIM
    empty_state = jnp.zeros((HEADS, HEAD_DIM, STATE), jnp.float32)

    def layer_pair(inputs, writes_one, reads_one, decay_one, skip_one, writes_two, reads_two, decay_two, skip_two):
        first_out = run_layer(inputs.astype(jnp.float32), writes_one.astype(jnp.float32), reads_one.astype(jnp.float32), decay_one.T, skip_one, empty_state)[0]
        lattice = jnp.zeros((CLIP_TOKENS, features), jnp.bfloat16).at[order_first].set(first_out.astype(jnp.bfloat16))
        second_in = lattice[order_second]
        return run_layer(second_in.astype(jnp.float32), writes_two.astype(jnp.float32), reads_two.astype(jnp.float32), decay_two.T, skip_two, empty_state)[0]

    def per_clip(pieces):
        inputs, writes_one, reads_one, decay_one, writes_two, reads_two, decay_two, upstream = pieces
        _, pullback = jax.vjp(layer_pair, inputs, writes_one, reads_one, decay_one, skip_first, writes_two, reads_two, decay_two, skip_second)
        return pullback(upstream)
    grads = lax.map(per_clip, (layer_input, writes_first, reads_first, decay_first, writes_second, reads_second, decay_second, cotangent))
    factor = 1.0 / math.sqrt(CLIP_COUNT * CLIP_TOKENS * HEAD_DIM)
    return (grads[0], grads[1], grads[2], grads[3], lax.optimization_barrier(jnp.sum(grads[4], axis=0)) * factor, grads[5], grads[6], grads[7], lax.optimization_barrier(jnp.sum(grads[8], axis=0)) * factor)
```

```python
import functools
import math
import types

import jax
import jax.numpy as jnp
from jax import lax
from jax.experimental import pallas as pl
from jax.experimental.pallas import tpu as pltpu
from jax.sharding import PartitionSpec as P

MESH = pl.DeviceIdType.MESH
HIGHEST = lax.Precision.HIGHEST
F32 = jnp.float32
BF16 = jnp.bfloat16


def nn(a, b, precision=None):
    return lax.dot_general(a, b, (((1,), (0,)), ((), ())), precision=precision, preferred_element_type=F32)


def nt(a, b, precision=None):
    return lax.dot_general(a, b, (((1,), (1,)), ((), ())), precision=precision, preferred_element_type=F32)


def tn(a, b, precision=None):
    return lax.dot_general(a, b, (((0,), (0,)), ((), ())), precision=precision, preferred_element_type=F32)


def iota(shape, dim):
    return lax.broadcasted_iota(jnp.int32, shape, dim)


def two(a):
    high = a.astype(BF16)
    return high, (a - high.astype(F32)).astype(BF16)


def rows_of(*parts):
    return jnp.concatenate(parts, axis=0)


def decay_sums(length):
    half, mid = length // 2, length // 4
    t, s = iota((length + 8, length), 0), iota((length + 8, length), 1)
    first, second = mid, half + mid
    middle = jnp.where(t < half, first, second)
    by_token = (s <= t).astype(F32) - (s < middle).astype(F32)
    k = t - length
    by_chunk = jnp.where(k == 0, (s < first).astype(F32), 0.0)
    by_chunk = jnp.where(k == 1, (s < second).astype(F32), by_chunk)
    by_chunk = jnp.where(k == 2, (s >= first).astype(F32), by_chunk)
    by_chunk = jnp.where(k == 3, (s >= second).astype(F32), by_chunk)
    by_chunk = jnp.where(k == 4, 1.0, by_chunk)
    by_chunk = jnp.where(k == 5, ((s >= first) & (s < second)).astype(F32), by_chunk)
    return jnp.where(k < 0, by_token, by_chunk).astype(BF16)


def factors(log_decay, size):
    heads, length = log_decay.shape
    sums = decay_sums(length)
    wide = [
        jnp.concatenate([jnp.broadcast_to(part[h : h + 1], (size, length)) for h in range(heads)], axis=0).astype(BF16)
        for part in (p.astype(F32) for p in two(log_decay))
    ]
    logs = nt(sums, wide[0]) + nt(sums, wide[1])
    by_token = logs[:length]
    return jnp.exp(by_token), jnp.exp(-by_token), jnp.exp(logs[length:])


def strict_scores(a, b, lower):
    scores = nt(a, b)
    row, col = iota(scores.shape, 0), iota(scores.shape, 1)
    return two(jnp.where(row > col if lower else row < col, scores, 0.0))


def lead(left, scores, low, start, first, second, starts_low=None, parts_low=None):
    both = rows_of(first, second)
    out = nn(jnp.concatenate([left, scores], axis=1), rows_of(start, both))
    if low is not None:
        out = out + nn(low, both)
    if starts_low is not None:
        out = out + nn(jnp.concatenate([left, scores], axis=1), rows_of(starts_low, *parts_low))
    return out


def whole_kernel(n, clips, size, held, sems, *refs):
    x = types.SimpleNamespace(**dict(zip(held, refs[20:])))
    x.u, x.w1, x.r1, x.g1, x.k1, x.w2, x.r2, x.g2, x.k2, x.o1, x.o2, x.ct = refs[:12]
    x.dinput, x.dw1, x.dr1, x.dw2, x.dr2, x.decays1_in, x.decays2_in, x.parts_in = refs[12:20]
    x.__dict__.update(zip(sems, zip(refs[20 + len(held) :: 2], refs[21 + len(held) :: 2])))
    me, clip = lax.axis_index("seq"), lax.axis_index("dp")
    chips = n // 2
    chip, core = lax.div(me, 2), lax.rem(me, 2)
    twin = me + 1 - 2 * core
    heads, length = x.g1.shape[1:]
    features = heads * size
    half = length // 2
    here = pl.ds(pl.multiple_of(me * features, features), features)

    def chunk(b):
        return pl.ds(pl.multiple_of(b * length, length), length)

    barrier = pltpu.get_barrier_semaphore()
    for d in range(1, n):
        pl.semaphore_signal(barrier, inc=1, device_id={"seq": lax.rem(me + d, n)}, device_id_type=MESH)
    for d in range(1, clips):
        pl.semaphore_signal(barrier, inc=1, device_id={"dp": lax.rem(clip + d, clips)}, device_id_type=MESH)
    x.ct_out[...] = x.ct[...].astype(BF16)
    pl.semaphore_wait(barrier, n + clips - 2)

    def copy_to(axis, to, src, dst, pair, *at):
        return pltpu.make_async_remote_copy(
            src_ref=src,
            dst_ref=dst,
            send_sem=pair[0].at[at],
            recv_sem=pair[1].at[at],
            device_id={axis: to},
            device_id_type=MESH,
        )

    def cut(ref, at):
        return ref.at[:, pl.ds(pl.multiple_of(at * features, features), features)]

    def device(away, other):
        return 2 * lax.rem(chip + away, chips) + (1 - core if other else core)

    peers = [(away, other) for away in range(1, chips) for other in (0, 1)] + [(0, 1)]
    moves = [
        lambda to: (x.g2.at[to], x.g_all.at[1, me]),
        lambda to: (cut(x.ct_out, to), x.ct_all.at[me]),
        lambda to: (x.g1.at[to], x.g_all.at[0, me]),
        lambda to: (cut(x.u, to), x.u_all.at[me]),
        lambda to: (x.o1, x.o1_all.at[me]),
        lambda to: (x.o2, x.o2_all.at[me]),
    ]
    arriving = [[] for _ in moves]

    def issue(k):
        for away, other in peers:
            to = device(away, other)
            copy = copy_to("seq", to, *moves[k](to), x.move, 2 * away + other - 1, k)
            copy.start()
            arriving[k].append(copy)

    pairs = ((x.w2, x.w_all.at[1]), (x.r2, x.r_all.at[1]), (x.w1, x.w_all.at[0]), (x.r1, x.r_all.at[0]))
    far, near = [], []

    def issue_pair(k):
        src, dst = pairs[k]
        for away in range(1, chips):
            copy = copy_to("seq", device(away, 0), src, dst.at[me], x.near, away - 1, k)
            copy.start()
            far.append(copy)
        copy = copy_to("seq", twin, src, dst.at[me], x.near, chips - 1, k)
        copy.start()
        near.append(copy)

    def wait_for(k):
        for copy in arriving[k]:
            copy.wait_recv()

    issue_pair(0)
    issue_pair(1)
    issue(0)
    issue(2)
    issue_pair(2)
    issue_pair(3)
    issue(4)
    issue(5)
    issue(1)
    issue(3)
    x.g_all[0, me] = x.g1[me]
    x.g_all[1, me] = x.g2[me]
    for src, dst in pairs + ((x.o1, x.o1_all), (x.o2, x.o2_all)):
        dst[me] = src[...]
    x.u_all[me] = x.u[:, here]
    x.ct_all[me] = x.ct_out[:, here]

    first = me * heads

    def gains(ref):
        channel = iota((1, features), 1) // size
        row = jnp.zeros((1, features), F32)
        for h in range(heads):
            row = jnp.where(channel == h, ref[first + h], row)
        return row

    skips = (gains(x.k1), gains(x.k2))

    def prepare_decays(layer):
        def step(b, carry):
            grown, shrunk, sums = factors(x.g_all[layer, b], size)
            x.grown[layer, b] = grown
            x.shrunk[layer, b] = shrunk
            x.sums[layer, b] = sums
            return carry

        lax.fori_loop(0, n, step, 0)

    def prepare_scores(layer):
        def step(b, carry):
            w, r = x.w_all[layer, b], x.r_all[layer, b]
            x.fore[layer, b], x.fore_low[layer, b] = strict_scores(r, w, True)
            x.back[layer, b], x.back_low[layer, b] = strict_scores(w, r, False)
            return carry

        lax.fori_loop(0, n, step, 0)

    def prepare_order(src, dst, out):
        def step(i, carry):
            cell = jnp.transpose(jnp.broadcast_to(dst[i].astype(F32), (length, length)))
            out[i] = jnp.concatenate([(cell == src[j].astype(F32)).astype(BF16) for j in range(n)], axis=1)
            return carry

        lax.fori_loop(0, n, step, 0)

    wait_for(0)
    prepare_decays(1)
    wait_for(2)
    prepare_decays(0)
    for copy in far:
        copy.wait_recv()
    for k, (src, dst) in enumerate(pairs):
        for away in range(1, chips):
            block = 2 * lax.rem(chip - away + chips, chips) + core
            copy = copy_to("seq", twin, dst.at[block], dst.at[block], x.near, chips - 1 + away, k)
            copy.start()
            near.append(copy)
    wait_for(4)
    wait_for(5)
    prepare_order(x.o2_all, x.o1_all, x.take_first)
    prepare_order(x.o1_all, x.o2_all, x.take_second)
    for copy in near:
        copy.wait_recv()
    prepare_scores(1)
    prepare_scores(0)
    state, adjoint = x.state, x.adjoint
    adjoint[...] = jnp.zeros_like(adjoint)
    state[...] = jnp.zeros_like(state)

    def own(w, r):
        return jnp.sum(w.astype(F32) * r.astype(F32), axis=1, keepdims=True)

    def back(layer, b, dy):
        wide, w, r = dy.astype(F32), x.w_all[layer, b], x.r_all[layer, b]
        sums, scores, low = x.sums[layer, b], x.back[layer, b], x.back_low[layer, b]
        scaled = wide * x.grown[layer, b]
        high = scaled.astype(BF16)
        a, z = high[:half], high[half:]
        turned = (scaled[half:] * sums[5:6]).astype(BF16)
        end = adjoint[...]
        end_a, end_z = (end * sums[2:3]).astype(BF16), (end * sums[3:4]).astype(BF16)
        x.ends[layer, b] = end
        x.ends_a[layer, b] = end_a
        x.ends_z[layer, b] = end_z
        x.dys[layer, b] = high
        top = lead(w[:half], scores[:half], low[:half], end_a, a, turned)
        bottom = lead(w[half:], scores[half:], low[half:], end_z, a, z)
        inner = rows_of(top, bottom) * x.shrunk[layer, b]
        x.inner[layer, b] = inner
        carried = rows_of(scaled[:half] * sums[0:1], scaled[half:] * sums[1:2]).astype(BF16)
        adjoint[...] = end * sums[4:5] + tn(r, carried)
        return inner + (skips[layer] + own(w, r)) * wide

    lower = iota((length, length), 0) >= iota((length, length), 1)
    since = lower.astype(BF16)
    picks = (iota((features, heads), 0) // size == iota((features, heads), 1)).astype(BF16)

    def forward(layer, b, u, dy, precise):
        wide, wide_dy, w, r = u.astype(F32), dy.astype(F32), x.w_all[layer, b], x.r_all[layer, b]
        sums, scores, low = x.sums[layer, b], x.fore[layer, b], x.fore_low[layer, b]
        scaled = wide * x.shrunk[layer, b]
        high, rest = two(scaled)
        a, z, a_low, z_low = high[:half], high[half:], rest[:half], rest[half:]
        turned, turned_low = two(scaled[:half] * sums[5:6])
        start = state[...]
        start_a, start_a_low = two(start * sums[0:1])
        start_z, start_z_low = two(start * sums[1:2])
        if precise:
            top = lead(r[:half], scores[:half], low[:half], start_a, a, z, start_a_low, (a_low, z_low))
            bottom = lead(r[half:], scores[half:], low[half:], start_z, turned, z, start_z_low, (turned_low, z_low))
        else:
            top = lead(r[:half], scores[:half], None, start_a, a, z)
            bottom = lead(r[half:], scores[half:], None, start_z, turned, z)
        inner = rows_of(top, bottom) * x.grown[layer, b]
        carried, carried_low = two(rows_of(scaled[:half] * sums[2:3], scaled[half:] * sums[3:4]))
        after = start * sums[4:5] + tn(w, carried)
        if precise:
            after = after + tn(w, carried_low)
        state[...] = after

        through = jnp.sum(x.ends[layer, b] * after, axis=0, keepdims=True)
        terms = wide_dy * inner - wide * x.inner[layer, b]
        last = terms[length - 8 :] + jnp.where(iota((8, features), 0) == 7, through, 0.0)
        terms, terms_low = two(rows_of(terms[: length - 8], last))
        by_head, by_head_low = two(nn(terms, picks) + nn(terms_low, picks))
        ddecay = tn(by_head, since) + tn(by_head_low, since)

        dys = x.dys[layer, b]
        dy_a, dy_z = dys[:half], dys[half:]
        dscores = rows_of(
            nt(dy_a, high) + nt(dy_a, rest),
            nt(dy_z, rows_of(turned, z)) + nt(dy_z, rows_of(turned_low, z_low)),
        )
        dscores, dscores_low = two(jnp.where(lower, dscores, 0.0))
        dreads = nn(dscores, w) + nn(dscores_low, w) + rows_of(nt(dy_a, start_a), nt(dy_z, start_z))
        dwrites = (
            tn(dscores, r)
            + tn(dscores_low, r)
            + rows_of(nt(a, x.ends_a[layer, b]), nt(z, x.ends_z[layer, b]))
        )
        x.params[layer, b, 0] = dwrites
        x.params[layer, b, 1] = dreads
        x.decays[layer, b] = ddecay
        return inner + (skips[layer] + own(w, r)) * wide

    decays_in = (x.decays1_in, x.decays2_in)

    def input_copy(to, slot):
        return copy_to("seq", to, x.du1.at[to], x.dinput.at[:, here], x.input, slot)

    def decay_copy(layer, to, slot):
        return copy_to("seq", to, x.decays.at[layer, to], decays_in[layer].at[me], x.decay, layer, slot)

    def twin_copy(layer, owner, slot):
        return copy_to("seq", twin, x.params.at[layer, owner], x.twins.at[layer, slot], x.twin, layer, slot)

    def slot_of(to):
        return lax.rem(to - me + n, n) - 1

    def leave(layer, b):
        @pl.when(b != me)
        def _():
            decay_copy(layer, b, slot_of(b)).start()

        @pl.when(lax.rem(b, 2) != core)
        def _():
            twin_copy(layer, b, lax.rem(lax.div(b, 2) - chip + chips, chips)).start()

    chip_copies = []

    def leave_chip(layer):
        for away in range(1, chips):
            owner = device(away, 0)
            twin_copy(layer, device(away, 1), away).wait_recv()
            total = x.params[layer, owner] + x.twins[layer, away]
            x.chip_sums[layer, away] = total.astype(BF16)
            copy = copy_to(
                "seq", owner, x.chip_sums.at[layer, away], x.chips_in.at[layer, away], x.chip, layer, away
            )
            copy.start()
            chip_copies.append(copy)

    wait_for(1)

    def back_second(i, carry):
        b = n - 1 - i
        x.du2[chunk(b)] = back(1, b, x.ct_all[b]).astype(BF16)
        return carry

    lax.fori_loop(0, n, back_second, 0, unroll=2)

    def regrid_back(i, carry):
        x.dy1[chunk(i)] = nn(x.take_first[i], x.du2[...]).astype(BF16)
        return carry

    lax.fori_loop(0, n, regrid_back, 0, unroll=2)
    adjoint[...] = jnp.zeros_like(adjoint)

    def back_first(i, carry):
        b = n - 1 - i
        x.du1[b] = back(0, b, x.dy1[chunk(b)]).astype(BF16)

        @pl.when(b != me)
        def _():
            input_copy(b, slot_of(b)).start()

        return carry

    lax.fori_loop(0, n, back_first, 0)
    wait_for(3)
    x.skips[...] = jnp.zeros_like(x.skips)

    def first_layer(b, carry):
        u, dy = x.u_all[b], x.dy1[chunk(b)]
        x.y1[chunk(b)] = forward(0, b, u, dy, True).astype(BF16)
        x.skips[0:1, :] += jnp.sum(u.astype(F32) * dy.astype(F32), axis=0, keepdims=True)
        leave(0, b)
        return carry

    lax.fori_loop(0, n, first_layer, 0)

    def regrid(i, carry):
        u = nn(x.take_second[i], x.y1[...])
        x.u2[i] = u.astype(BF16)
        x.skips[1:2, :] += jnp.sum(u * x.ct_all[i].astype(F32), axis=0, keepdims=True)
        return carry

    lax.fori_loop(0, n, regrid, 0, unroll=2)
    clip_copies = []
    for d in range(1, clips):
        to = lax.rem(clip + d, clips)
        copy = copy_to("dp", to, x.skips, x.clips_in.at[clip], x.clip, d - 1)
        copy.start()
        clip_copies.append(copy)
    x.clips_in[clip] = x.skips[...]
    leave_chip(0)
    state[...] = jnp.zeros_like(state)

    def second_layer(b, carry):
        forward(1, b, x.u2[b], x.ct_all[b], False)
        leave(1, b)
        return carry

    lax.fori_loop(0, n, second_layer, 0)
    for copy in clip_copies:
        copy.wait()
    x.summed[...] = jnp.sum(x.clips_in[...], axis=0)
    last = []
    for d in range(1, n):
        to = lax.rem(me + d, n)
        copy = copy_to("seq", to, x.summed, x.parts_in.at[me], x.part, d - 1)
        copy.start()
        last.append(copy)
    leave_chip(1)
    x.parts_in[me] = x.summed[...]
    for layer in range(2):
        decays_in[layer][me] = x.decays[layer, me]
    x.dinput[:, here] = x.du1[me]
    for layer, outs in enumerate(((x.dw1, x.dr1), (x.dw2, x.dr2))):
        twin_copy(layer, twin, 0).wait_recv()
        for k, out in enumerate(outs):
            total = x.params[layer, me, k] + x.twins[layer, 0, k]
            if k == 0:
                for copy in chip_copies[layer * (chips - 1) : (layer + 1) * (chips - 1)]:
                    copy.wait_recv()
            for away in range(1, chips):
                total = total + x.chips_in[layer, away, k].astype(F32)
            out[...] = total.astype(BF16)
    for group in arriving:
        for copy in group:
            copy.wait_send()
    for copy in far + near + chip_copies:
        copy.wait_send()
    for layer in range(2):
        for away in range(chips):
            twin_copy(layer, device(away, 1), away).wait_send()
    for d in range(1, n):
        to = lax.rem(me + d, n)
        last += [input_copy(to, d - 1), decay_copy(0, to, d - 1), decay_copy(1, to, d - 1)]
    for copy in last:
        copy.wait()


def whole(n, clips, size, *args):
    length, width = args[0].shape
    heads = args[3].shape[1]
    count = args[1].shape[1]
    features, half, chips = heads * size, length // 2, n // 2
    vmem = pl.BlockSpec(memory_space=pltpu.VMEM)
    smem = pl.BlockSpec(memory_space=pltpu.SMEM)
    param, decay, gain = (length, count), (n, heads, length), (2, features)
    wide, flat, held, square = (n, length, features), (n * length, features), (n, count, features), (n, length, length)
    order, pick, pair = (n, 1, length), (n, length, n * length), (2, length, count)
    outs = (((length, width), BF16),) + ((param, BF16),) * 4 + ((decay, F32),) * 2 + (((n,) + gain, F32),)
    scratch = dict(
        ct_out=((length, width), BF16),
        u_all=(wide, BF16),
        ct_all=(wide, BF16),
        w_all=((2, n) + param, BF16),
        r_all=((2, n) + param, BF16),
        g_all=((2,) + decay, F32),
        o1_all=(order, jnp.int32),
        o2_all=(order, jnp.int32),
        grown=((2,) + wide, F32),
        shrunk=((2,) + wide, F32),
        sums=((2, n, 8, features), F32),
        fore=((2,) + square, BF16),
        fore_low=((2,) + square, BF16),
        back=((2,) + square, BF16),
        back_low=((2,) + square, BF16),
        take_first=(pick, BF16),
        take_second=(pick, BF16),
        du2=(flat, BF16),
        dy1=(flat, BF16),
        y1=(flat, BF16),
        u2=(wide, BF16),
        du1=(wide, BF16),
        dys=((2,) + wide, BF16),
        ends=((2,) + held, F32),
        ends_a=((2,) + held, BF16),
        ends_z=((2,) + held, BF16),
        inner=((2,) + wide, F32),
        state=((count, features), F32),
        adjoint=((count, features), F32),
        params=((2, n) + pair, F32),
        twins=((2, chips) + pair, F32),
        chip_sums=((2, chips) + pair, BF16),
        chips_in=((2, chips) + pair, BF16),
        decays=((2,) + decay, F32),
        skips=(gain, F32),
        clips_in=((clips,) + gain, F32),
        summed=(gain, F32),
    )
    sems = dict(
        move=(n - 1, 6),
        near=(n - 1, 4),
        input=(n - 1,),
        decay=(2, n - 1),
        twin=(2, chips),
        chip=(2, chips),
        clip=(clips - 1,),
        part=(n - 1,),
    )
    return pl.pallas_call(
        functools.partial(whole_kernel, n, clips, size, tuple(scratch), tuple(sems)),
        out_shape=tuple(jax.ShapeDtypeStruct(*out) for out in outs),
        in_specs=[vmem] * 4 + [smem] + [vmem] * 3 + [smem] + [vmem] * 3,
        out_specs=[vmem] * 8,
        scratch_shapes=[pltpu.VMEM(*one) for one in scratch.values()]
        + [pltpu.SemaphoreType.DMA(shape) for shape in sems.values() for _ in range(2)],
        compiler_params=pltpu.CompilerParams(collective_id=0, has_side_effects=True),
        name="whole",
    )(*args)


def gather_kernel(n, factor, *refs):
    parts = refs[7]
    for src, dst in zip(refs[:7], refs[8:15]):
        dst[...] = src[...]
    dk1, dk2 = refs[15:]
    heads = refs[5].shape[1]
    width = parts.shape[2]
    size = width // heads
    picks = (iota((width, heads), 0) // size == iota((width, heads), 1)).astype(F32)
    for s in range(n):
        by_head = nn(parts[s], picks, HIGHEST) * factor
        dk1[:, s * heads : (s + 1) * heads] = by_head[0:1]
        dk2[:, s * heads : (s + 1) * heads] = by_head[1:2]


def gather(n, factor, *results):
    heads = results[5].shape[1]
    vmem = pl.BlockSpec(memory_space=pltpu.VMEM)
    skip = jax.ShapeDtypeStruct((1, n * heads), F32)
    return pl.pallas_call(
        functools.partial(gather_kernel, n, factor),
        out_shape=tuple(jax.ShapeDtypeStruct(one.shape, one.dtype) for one in results[:7]) + (skip, skip),
        in_specs=[vmem] * 8,
        out_specs=[vmem] * 9,
        name="gather",
    )(*results)


def on_device(n, clips, u, w1, r1, g1, k1, w2, r2, g2, k2, o1, o2, ct):
    length, features = u.shape[1:]
    head_count = k1.shape[0]
    size = features // head_count
    heads = head_count // n

    def by_device(g):
        return g.reshape(n, heads, length)

    results = whole(
        n,
        clips,
        size,
        u[0],
        w1[0],
        r1[0],
        by_device(g1),
        k1,
        w2[0],
        r2[0],
        by_device(g2),
        k2,
        o1[None],
        o2[None],
        ct[0],
    )
    factor = 1.0 / math.sqrt(clips * n * length * size)
    du, dw1, dr1, dw2, dr2, dg1, dg2, dk1, dk2 = gather(n, factor, *results)
    return (
        du[None],
        dw1[None],
        dr1[None],
        dg1.reshape(1, head_count, length),
        dk1[0],
        dw2[None],
        dr2[None],
        dg2.reshape(1, head_count, length),
        dk2[0],
    )


def solution(mesh):
    tokens, decay = P("dp", "seq", None), P("dp", None, "seq")
    return jax.shard_map(
        functools.partial(on_device, mesh.shape["seq"], mesh.shape["dp"]),
        mesh=mesh,
        in_specs=(tokens, tokens, tokens, decay, P(), tokens, tokens, decay, P(), P("seq"), P("seq"), tokens),
        out_specs=(tokens, tokens, tokens, decay, P(), tokens, tokens, decay, P()),
        check_vma=False,
    )
```

```python
import functools
import math
import types

import jax
import jax.numpy as jnp
from jax import lax
from jax.experimental import pallas as pl
from jax.experimental.pallas import tpu as pltpu
from jax.sharding import PartitionSpec as P

MESH = pl.DeviceIdType.MESH
HIGHEST = lax.Precision.HIGHEST
F32 = jnp.float32
BF16 = jnp.bfloat16


def nn(a, b, precision=None):
    return lax.dot_general(a, b, (((1,), (0,)), ((), ())), precision=precision, preferred_element_type=F32)


def nt(a, b, precision=None):
    return lax.dot_general(a, b, (((1,), (1,)), ((), ())), precision=precision, preferred_element_type=F32)


def tn(a, b, precision=None):
    return lax.dot_general(a, b, (((0,), (0,)), ((), ())), precision=precision, preferred_element_type=F32)


def iota(shape, dim):
    return lax.broadcasted_iota(jnp.int32, shape, dim)


def two(a):
    high = a.astype(BF16)
    return high, (a - high.astype(F32)).astype(BF16)


def rows_of(*parts):
    return jnp.concatenate(parts, axis=0)


def decay_sums(length):
    half, mid = length // 2, length // 4
    t, s = iota((length + 8, length), 0), iota((length + 8, length), 1)
    first, second = mid, half + mid
    middle = jnp.where(t < half, first, second)
    by_token = (s <= t).astype(F32) - (s < middle).astype(F32)
    k = t - length
    by_chunk = jnp.where(k == 0, (s < first).astype(F32), 0.0)
    by_chunk = jnp.where(k == 1, (s < second).astype(F32), by_chunk)
    by_chunk = jnp.where(k == 2, (s >= first).astype(F32), by_chunk)
    by_chunk = jnp.where(k == 3, (s >= second).astype(F32), by_chunk)
    by_chunk = jnp.where(k == 4, 1.0, by_chunk)
    by_chunk = jnp.where(k == 5, ((s >= first) & (s < second)).astype(F32), by_chunk)
    return jnp.where(k < 0, by_token, by_chunk).astype(BF16)


def factors(log_decay, size):
    heads, length = log_decay.shape
    sums = decay_sums(length)
    wide = [
        jnp.concatenate([jnp.broadcast_to(part[h : h + 1], (size, length)) for h in range(heads)], axis=0).astype(BF16)
        for part in (p.astype(F32) for p in two(log_decay))
    ]
    logs = nt(sums, wide[0]) + nt(sums, wide[1])
    by_token = logs[:length]
    return jnp.exp(by_token), jnp.exp(-by_token), jnp.exp(logs[length:])


def strict_scores(a, b, lower):
    scores = nt(a, b)
    row, col = iota(scores.shape, 0), iota(scores.shape, 1)
    return two(jnp.where(row > col if lower else row < col, scores, 0.0))


def whole_kernel(n, clips, size, held, sems, *refs):
    x = types.SimpleNamespace(**dict(zip(held, refs[20:])))
    x.u, x.w1, x.r1, x.g1, x.k1, x.w2, x.r2, x.g2, x.k2, x.o1, x.o2, x.ct = refs[:12]
    x.dinput, x.dw1, x.dr1, x.dw2, x.dr2, x.decays1_in, x.decays2_in, x.parts_in = refs[12:20]
    x.load, x.rounds = refs[-2:]
    x.__dict__.update(zip(sems, zip(refs[20 + len(held) : -2 : 2], refs[21 + len(held) : -2 : 2])))
    me, clip = lax.axis_index("seq"), lax.axis_index("dp")
    chips = n // 2
    chip, core = lax.div(me, 2), lax.rem(me, 2)
    twin = me + 1 - 2 * core
    heads, length = x.g1.shape[1:]
    features = heads * size
    half = length // 2
    here = pl.ds(pl.multiple_of(me * features, features), features)

    def chunk(b):
        return pl.ds(pl.multiple_of(b * length, length), length)

    def cut(ref, at):
        return ref.at[:, pl.ds(pl.multiple_of(at * features, features), features)]

    barrier = pltpu.get_barrier_semaphore()
    for d in range(1, n):
        pl.semaphore_signal(barrier, inc=1, device_id={"seq": lax.rem(me + d, n)}, device_id_type=MESH)
    lines = ((clip >= 0, clip + 1 - 2 * lax.rem(clip, 2)), (clip >= 2, clip - 2), (clip < clips - 2, clip + 2))
    greetings = sum(jnp.where(there, 1, 0) for there, _ in lines)

    def greet(sem):
        for there, to in lines:

            @pl.when(there)
            def _():
                pl.semaphore_signal(sem, inc=1, device_id={"dp": to}, device_id_type=MESH)

    met = []

    def hear(count):
        for k in range(len(met), count):
            pl.semaphore_wait(x.rounds.at[k], greetings)
            met.append(k)
            if k + 1 < clips // 2 - 1:
                greet(x.rounds.at[k + 1])

    greet(barrier)
    load = pltpu.make_async_copy(x.ct, x.ct_wide, x.load.at[0])
    load.start()
    own_load = pltpu.make_async_copy(cut(x.u, me), x.u_all.at[me], x.load.at[1])
    own_load.start()
    load.wait()
    x.ct_out[...] = x.ct_wide[...].astype(BF16)
    pl.semaphore_wait(barrier, n - 1 + greetings)
    greet(x.rounds.at[0])

    def copy_to(axis, to, src, dst, pair, *at):
        return pltpu.make_async_remote_copy(
            src_ref=src,
            dst_ref=dst,
            send_sem=pair[0].at[at],
            recv_sem=pair[1].at[at],
            device_id={axis: to},
            device_id_type=MESH,
        )

    def device(away, other):
        return 2 * lax.rem(chip + away, chips) + (1 - core if other else core)

    peers = [(away, other) for away in range(1, chips) for other in (0, 1)] + [(0, 1)]
    moves = [
        lambda to: (x.g2.at[to], x.g_all.at[1, me]),
        lambda to: (cut(x.ct_out, to), x.ct_all.at[chunk(me)]),
        lambda to: (x.g1.at[to], x.g_all.at[0, me]),
        lambda to: (cut(x.u, to), x.u_all.at[me]),
        lambda to: (x.o1, x.o1_all.at[me]),
        lambda to: (x.o2, x.o2_all.at[me]),
    ]
    arriving = [[] for _ in moves]

    def issue(k):
        for away, other in peers:
            to = device(away, other)
            copy = copy_to("seq", to, *moves[k](to), x.move, 2 * away + other - 1, k)
            copy.start()
            arriving[k].append(copy)

    pairs = ((x.w2, x.w_all.at[1]), (x.r2, x.r_all.at[1]), (x.w1, x.w_all.at[0]), (x.r1, x.r_all.at[0]))
    far, near = [], []

    def issue_pair(k):
        src, dst = pairs[k]
        for away in range(1, chips):
            copy = copy_to("seq", device(away, 0), src, dst.at[me], x.near, away - 1, k)
            copy.start()
            far.append(copy)
        copy = copy_to("seq", twin, src, dst.at[me], x.near, chips - 1, k)
        copy.start()
        near.append(copy)

    def wait_block(k, b):
        away = lax.rem(chip - lax.div(b, 2) + chips, chips)
        at = 2 * away + lax.rem(core + lax.rem(b, 2), 2) - 1
        src, dst = moves[k](b)
        copy_to("seq", b, src, dst, x.move, at, k).wait_recv()

    def wait_for(k):
        for copy in arriving[k]:
            copy.wait_recv()

    issue_pair(0)
    issue_pair(1)
    issue(0)
    issue(2)
    issue_pair(2)
    issue_pair(3)
    issue(4)
    issue(5)
    issue(1)
    issue(3)
    x.g_all[0, me] = x.g1[me]
    x.g_all[1, me] = x.g2[me]
    for src, dst in pairs + ((x.o1, x.o1_all), (x.o2, x.o2_all)):
        dst[me] = src[...]
    x.ct_all[chunk(me)] = x.ct_out[:, here]

    first = me * heads

    def gains(ref):
        channel = iota((1, features), 1) // size
        row = jnp.zeros((1, features), F32)
        for h in range(heads):
            row = jnp.where(channel == h, ref[first + h], row)
        return row

    skips = (gains(x.k1), gains(x.k2))

    def prepare_decays(layer):
        def step(b, carry):
            grown, shrunk, sums = factors(x.g_all[layer, b], size)
            x.grown[layer, b] = grown
            x.shrunk[layer, b] = shrunk
            x.sums[layer, b] = sums
            return carry

        lax.fori_loop(0, n, step, 0, unroll=4)

    def prepare_scores(layer):
        def step(b, carry):
            w, r = x.w_all[layer, b], x.r_all[layer, b]
            x.fore[layer, b], x.fore_low[layer, b] = strict_scores(r, w, True)
            x.back[layer, b], x.back_low[layer, b] = strict_scores(w, r, False)
            return carry

        lax.fori_loop(0, n, step, 0, unroll=4)

    def prepare_order(src, dst, out):
        def step(i, carry):
            cell = jnp.transpose(jnp.broadcast_to(dst[i].astype(F32), (length, length)))
            out[i] = jnp.concatenate([(cell == src[j].astype(F32)).astype(BF16) for j in range(n)], axis=1)
            return carry

        lax.fori_loop(0, n, step, 0, unroll=4)

    wait_for(0)
    hear(1)
    prepare_decays(1)
    wait_for(2)
    prepare_decays(0)
    for copy in far:
        copy.wait_recv()
    for k, (src, dst) in enumerate(pairs):
        for away in range(1, chips):
            block = 2 * lax.rem(chip - away + chips, chips) + core
            copy = copy_to("seq", twin, dst.at[block], dst.at[block], x.near, chips - 1 + away, k)
            copy.start()
            near.append(copy)
    wait_for(4)
    wait_for(5)
    prepare_order(x.o2_all, x.o1_all, x.take_first)
    prepare_order(x.o1_all, x.o2_all, x.take_second)
    for copy in near:
        copy.wait_recv()
    prepare_scores(1)
    prepare_scores(0)
    state, adjoint = x.state, x.adjoint
    adjoint[...] = jnp.zeros_like(adjoint)
    state[...] = jnp.zeros_like(state)

    def own(w, r):
        return jnp.sum(w.astype(F32) * r.astype(F32), axis=1, keepdims=True)

    step = min(2 * length, features)
    tiles = [slice(at, at + step) for at in range(0, features, step)]

    def back(layer, b, get, put):
        w, r = x.w_all[layer, b], x.r_all[layer, b]
        scores, low = x.back[layer, b], x.back_low[layer, b]
        left_a = jnp.concatenate([w[:half], scores[:half]], axis=1)
        left_z = jnp.concatenate([w[half:], scores[half:]], axis=1)
        diagonal = own(w, r)
        for lanes in tiles:
            wide, sums = get(lanes).astype(F32), x.sums[layer, b, :, lanes]
            scaled = wide * x.grown[layer, b, :, lanes]
            high = scaled.astype(BF16)
            a, z = high[:half], high[half:]
            x.dys[layer, b, :, lanes] = high
            turned = (scaled[half:] * sums[5:6]).astype(BF16)
            end = adjoint[:, lanes]
            carried = rows_of(scaled[:half] * sums[0:1], scaled[half:] * sums[1:2]).astype(BF16)
            adjoint[:, lanes] = end * sums[4:5] + tn(r, carried)
            end_a, end_z = (end * sums[2:3]).astype(BF16), (end * sums[3:4]).astype(BF16)
            x.ends[layer, b, :, lanes] = end
            x.ends_a[layer, b, :, lanes] = end_a
            x.ends_z[layer, b, :, lanes] = end_z
            top = nn(left_a, rows_of(end_a, a, turned)) + nn(low[:half], rows_of(a, turned))
            bottom = nn(left_z, rows_of(end_z, a, z)) + nn(low[half:], high)
            inner = rows_of(top, bottom) * x.shrunk[layer, b, :, lanes]
            x.inner[layer, b, :, lanes] = inner
            put(lanes, (inner + (skips[layer][:, lanes] + diagonal) * wide).astype(BF16))

    lower = iota((length, length), 0) >= iota((length, length), 1)
    since = lower.astype(BF16)
    picks = (iota((features, heads), 0) // size == iota((features, heads), 1)).astype(BF16)

    def forward(layer, b, get, put):
        w, r = x.w_all[layer, b], x.r_all[layer, b]
        scores, low = x.fore[layer, b], x.fore_low[layer, b]
        left_a = jnp.concatenate([r[:half], scores[:half]], axis=1)
        left_z = jnp.concatenate([r[half:], scores[half:]], axis=1)
        diagonal = own(w, r)
        for lanes in tiles:
            wide, sums = get(lanes).astype(F32), x.sums[layer, b, :, lanes]
            scaled = wide * x.shrunk[layer, b, :, lanes]
            high, rest = two(scaled)
            turned, turned_low = two(scaled[:half] * sums[5:6])
            start = state[:, lanes]
            carried, carried_low = two(rows_of(scaled[:half] * sums[2:3], scaled[half:] * sums[3:4]))
            after = start * sums[4:5] + tn(w, carried)
            if put:
                after = after + tn(w, carried_low)
            state[:, lanes] = after
            start_a, start_a_low = two(start * sums[0:1])
            start_z, start_z_low = two(start * sums[1:2])
            other, other_low = rows_of(turned, high[half:]), rows_of(turned_low, rest[half:])
            top = nn(left_a, rows_of(start_a, high))
            bottom = nn(left_z, rows_of(start_z, other))
            if put:
                top = top + nn(low[:half], high) + nn(left_a, rows_of(start_a_low, rest))
                bottom = bottom + nn(low[half:], other) + nn(left_z, rows_of(start_z_low, other_low))
            inner = rows_of(top, bottom) * x.grown[layer, b, :, lanes]
            if put:
                put(lanes, wide, (inner + (skips[layer][:, lanes] + diagonal) * wide).astype(BF16))
            x.us[layer, b, 0, :, lanes] = high
            x.us[layer, b, 1, :, lanes] = rest
            x.turns[layer, b, 0, :, lanes] = turned
            x.turns[layer, b, 1, :, lanes] = turned_low
            x.starts_a[layer, b, :, lanes] = start_a
            x.starts_z[layer, b, :, lanes] = start_z
            x.through[layer, b, :, lanes] = jnp.sum(x.ends[layer, b, :, lanes] * after, axis=0, keepdims=True)
            x.outer[layer, b, :, lanes] = inner

    def grads(layer, b, get, get_dy):
        w, r = x.w_all[layer, b], x.r_all[layer, b]
        totals = []
        for lanes in tiles:
            wide, wide_dy = get(lanes).astype(F32), get_dy(lanes).astype(F32)
            terms = wide_dy * x.outer[layer, b, :, lanes] - wide * x.inner[layer, b, :, lanes]
            through = jnp.where(iota((8, step), 0) == 7, x.through[layer, b, :, lanes], 0.0)
            terms, terms_low = two(rows_of(terms[: length - 8], terms[length - 8 :] + through))
            high, rest = x.us[layer, b, 0, :, lanes], x.us[layer, b, 1, :, lanes]
            other = rows_of(x.turns[layer, b, 0, :, lanes], high[half:])
            other_low = rows_of(x.turns[layer, b, 1, :, lanes], rest[half:])
            dys = x.dys[layer, b, :, lanes]
            dy_a, dy_z = dys[:half], dys[half:]
            parts = (
                nn(terms, picks[lanes]) + nn(terms_low, picks[lanes]),
                nt(dy_a, high) + nt(dy_a, rest),
                nt(dy_z, other) + nt(dy_z, other_low),
                nt(dy_a, x.starts_a[layer, b, :, lanes]),
                nt(dy_z, x.starts_z[layer, b, :, lanes]),
                nt(high[:half], x.ends_a[layer, b, :, lanes]),
                nt(high[half:], x.ends_z[layer, b, :, lanes]),
            )
            totals = [one + part for one, part in zip(totals, parts)] if totals else parts
        by_head, by_head_low = two(totals[0])
        x.decays[layer, b] = tn(by_head, since) + tn(by_head_low, since)
        dscores, dscores_low = two(jnp.where(lower, rows_of(*totals[1:3]), 0.0))
        x.params[layer, b, 0] = tn(dscores, r) + tn(dscores_low, r) + rows_of(*totals[5:7])
        x.params[layer, b, 1] = nn(dscores, w) + nn(dscores_low, w) + rows_of(*totals[3:5])

    decays_in = (x.decays1_in, x.decays2_in)

    def input_copy(to, slot):
        return copy_to("seq", to, x.du1.at[to], x.dinput.at[:, here], x.input, slot)

    def decay_copy(layer, to, slot):
        return copy_to("seq", to, x.decays.at[layer, to], decays_in[layer].at[me], x.decay, layer, slot)

    def twin_copy(layer, owner, slot):
        return copy_to("seq", twin, x.params.at[layer, owner], x.twins.at[layer, slot], x.twin, layer, slot)

    def slot_of(to):
        return lax.rem(to - me + n, n) - 1

    def leave(layer, b):
        @pl.when(b != me)
        def _():
            decay_copy(layer, b, slot_of(b)).start()

        @pl.when(lax.rem(b, 2) != core)
        def _():
            twin_copy(layer, b, lax.rem(lax.div(b, 2) - chip + chips, chips)).start()

    chip_copies = []

    def leave_chip(layer):
        for away in range(1, chips):
            owner = device(away, 0)
            twin_copy(layer, device(away, 1), away).wait_recv()
            total = x.params[layer, owner] + x.twins[layer, away]
            x.chip_sums[layer, away] = total.astype(BF16)
            copy = copy_to(
                "seq", owner, x.chip_sums.at[layer, away], x.chips_in.at[layer, away], x.chip, layer, away
            )
            copy.start()
            chip_copies.append(copy)

    hear(2)

    def back_second(i, carry):
        b = n - 1 - i

        @pl.when(b != me)
        def _():
            wait_block(1, b)

        def put(lanes, value):
            x.du2[chunk(b), lanes] = value

        back(1, b, lambda lanes: x.ct_all[chunk(b), lanes], put)
        return carry

    lax.fori_loop(0, n, back_second, 0, unroll=4)

    def regrid_back(i, carry):
        x.dy1[chunk(i)] = nn(x.take_first[i], x.du2[...]).astype(BF16)
        x.ct_first[chunk(i)] = nn(x.take_first[i], x.ct_all[...]).astype(BF16)
        return carry

    lax.fori_loop(0, n, regrid_back, 0, unroll=4)
    adjoint[...] = jnp.zeros_like(adjoint)

    def back_first(i, carry):
        b = n - 1 - i

        def put(lanes, value):
            x.du1[b, :, lanes] = value

        back(0, b, lambda lanes: x.dy1[chunk(b), lanes], put)

        @pl.when(b != me)
        def _():
            input_copy(b, slot_of(b)).start()

        return carry

    lax.fori_loop(0, n, back_first, 0, unroll=4)
    own_load.wait()
    hear(clips // 2 - 1)
    x.skips[...] = jnp.zeros_like(x.skips)

    def first_layer(b, carry):
        @pl.when(b != me)
        def _():
            wait_block(3, b)

        def put(lanes, wide, value):
            x.y1[chunk(b), lanes] = value
            x.skips[0:1, lanes] += jnp.sum(wide * x.dy1[chunk(b), lanes].astype(F32), axis=0, keepdims=True)
            upstream = x.ct_first[chunk(b), lanes].astype(F32)
            x.skips[1:2, lanes] += jnp.sum(value.astype(F32) * upstream, axis=0, keepdims=True)

        forward(0, b, lambda lanes: x.u_all[b, :, lanes], put)
        return carry

    lax.fori_loop(0, n, first_layer, 0, unroll=4)
    clip_copies = []
    for d in range(1, clips):
        to = lax.rem(clip + d, clips)
        copy = copy_to("dp", to, x.skips, x.clips_in.at[clip], x.clip, d - 1)
        copy.start()
        clip_copies.append(copy)
    x.clips_in[clip] = x.skips[...]

    def first_grads(b, carry):
        grads(0, b, lambda lanes: x.u_all[b, :, lanes], lambda lanes: x.dy1[chunk(b), lanes])
        leave(0, b)
        return carry

    lax.fori_loop(0, n, first_grads, 0, unroll=4)

    def regrid(i, carry):
        x.u2[i] = nn(x.take_second[i], x.y1[...]).astype(BF16)
        return carry

    lax.fori_loop(0, n, regrid, 0, unroll=4)
    leave_chip(0)
    state[...] = jnp.zeros_like(state)

    def second_layer(b, carry):
        forward(1, b, lambda lanes: x.u2[b, :, lanes], None)
        grads(1, b, lambda lanes: x.u2[b, :, lanes], lambda lanes: x.ct_all[chunk(b), lanes])
        leave(1, b)
        return carry

    lax.fori_loop(0, n, second_layer, 0, unroll=4)
    for copy in clip_copies:
        copy.wait()
    x.summed[...] = jnp.sum(x.clips_in[...], axis=0)
    last = []
    for d in range(1, n):
        to = lax.rem(me + d, n)
        copy = copy_to("seq", to, x.summed, x.parts_in.at[me], x.part, d - 1)
        copy.start()
        last.append(copy)
    leave_chip(1)
    x.parts_in[me] = x.summed[...]
    for layer in range(2):
        decays_in[layer][me] = x.decays[layer, me]
    x.dinput[:, here] = x.du1[me]
    for layer, outs in enumerate(((x.dw1, x.dr1), (x.dw2, x.dr2))):
        twin_copy(layer, twin, 0).wait_recv()
        for k, out in enumerate(outs):
            total = x.params[layer, me, k] + x.twins[layer, 0, k]
            if k == 0:
                for copy in chip_copies[layer * (chips - 1) : (layer + 1) * (chips - 1)]:
                    copy.wait_recv()
            for away in range(1, chips):
                total = total + x.chips_in[layer, away, k].astype(F32)
            out[...] = total.astype(BF16)
    for group in arriving:
        for copy in group:
            copy.wait_send()
    for copy in far + near + chip_copies:
        copy.wait_send()
    for layer in range(2):
        for away in range(chips):
            twin_copy(layer, device(away, 1), away).wait_send()
    for d in range(1, n):
        to = lax.rem(me + d, n)
        last += [input_copy(to, d - 1), decay_copy(0, to, d - 1), decay_copy(1, to, d - 1)]
    for copy in last:
        copy.wait()


def whole(n, clips, size, *args):
    length, width = args[0].shape
    heads = args[3].shape[1]
    count = args[1].shape[1]
    features, half, chips = heads * size, length // 2, n // 2
    vmem = pl.BlockSpec(memory_space=pltpu.VMEM)
    smem = pl.BlockSpec(memory_space=pltpu.SMEM)
    away = pl.BlockSpec(memory_space=pl.ANY)
    param, decay, gain = (length, count), (n, heads, length), (2, features)
    wide, flat, held, square = (n, length, features), (n * length, features), (n, count, features), (n, length, length)
    order, pick, pair = (n, 1, length), (n, length, n * length), (2, length, count)
    outs = (((length, width), BF16),) + ((param, BF16),) * 4 + ((decay, F32),) * 2 + (((n,) + gain, F32),)
    scratch = dict(
        ct_out=((length, width), BF16),
        ct_wide=((length, width), F32),
        u_all=(wide, BF16),
        ct_all=(flat, BF16),
        ct_first=(flat, BF16),
        w_all=((2, n) + param, BF16),
        r_all=((2, n) + param, BF16),
        g_all=((2,) + decay, F32),
        o1_all=(order, jnp.int32),
        o2_all=(order, jnp.int32),
        grown=((2,) + wide, F32),
        shrunk=((2,) + wide, F32),
        sums=((2, n, 8, features), F32),
        fore=((2,) + square, BF16),
        fore_low=((2,) + square, BF16),
        back=((2,) + square, BF16),
        back_low=((2,) + square, BF16),
        take_first=(pick, BF16),
        take_second=(pick, BF16),
        du2=(flat, BF16),
        dy1=(flat, BF16),
        y1=(flat, BF16),
        u2=(wide, BF16),
        du1=(wide, BF16),
        dys=((2,) + wide, BF16),
        ends=((2,) + held, F32),
        ends_a=((2,) + held, BF16),
        ends_z=((2,) + held, BF16),
        inner=((2,) + wide, F32),
        outer=((2,) + wide, F32),
        us=((2, n, 2, length, features), BF16),
        turns=((2, n, 2, half, features), BF16),
        starts_a=((2,) + held, BF16),
        starts_z=((2,) + held, BF16),
        through=((2, n, 1, features), F32),
        state=((count, features), F32),
        adjoint=((count, features), F32),
        params=((2, n) + pair, F32),
        twins=((2, chips) + pair, F32),
        chip_sums=((2, chips) + pair, BF16),
        chips_in=((2, chips) + pair, BF16),
        decays=((2,) + decay, F32),
        skips=(gain, F32),
        clips_in=((clips,) + gain, F32),
        summed=(gain, F32),
    )
    sems = dict(
        move=(n - 1, 6),
        near=(n - 1, 4),
        input=(n - 1,),
        decay=(2, n - 1),
        twin=(2, chips),
        chip=(2, chips),
        clip=(clips - 1,),
        part=(n - 1,),
    )
    taken = sum(math.prod(shape) * jnp.dtype(kind).itemsize for shape, kind in scratch.values())
    return pl.pallas_call(
        functools.partial(whole_kernel, n, clips, size, tuple(scratch), tuple(sems)),
        out_shape=tuple(jax.ShapeDtypeStruct(*out) for out in outs),
        in_specs=[away] + [vmem] * 3 + [smem] + [vmem] * 3 + [smem] + [vmem] * 2 + [away],
        out_specs=[vmem] * 8,
        scratch_shapes=[pltpu.VMEM(*one) for one in scratch.values()]
        + [pltpu.SemaphoreType.DMA(shape) for shape in sems.values() for _ in range(2)]
        + [pltpu.SemaphoreType.DMA((2,)), pltpu.SemaphoreType.REGULAR((clips // 2 - 1,))],
        compiler_params=pltpu.CompilerParams(
            collective_id=0, has_side_effects=True
        ),
        name="whole",
    )(*args)


def gather_kernel(n, factor, *refs):
    parts = refs[7]
    for src, dst in zip(refs[:7], refs[8:15]):
        dst[...] = src[...]
    dk1, dk2 = refs[15:]
    heads = refs[5].shape[1]
    width = parts.shape[2]
    size = width // heads
    picks = (iota((width, heads), 0) // size == iota((width, heads), 1)).astype(F32)
    for s in range(n):
        by_head = nn(parts[s], picks, HIGHEST) * factor
        dk1[:, s * heads : (s + 1) * heads] = by_head[0:1]
        dk2[:, s * heads : (s + 1) * heads] = by_head[1:2]


def gather(n, factor, *results):
    heads = results[5].shape[1]
    vmem = pl.BlockSpec(memory_space=pltpu.VMEM)
    skip = jax.ShapeDtypeStruct((1, n * heads), F32)
    return pl.pallas_call(
        functools.partial(gather_kernel, n, factor),
        out_shape=tuple(jax.ShapeDtypeStruct(one.shape, one.dtype) for one in results[:7]) + (skip, skip),
        in_specs=[vmem] * 8,
        out_specs=[vmem] * 9,
        name="gather",
    )(*results)


def on_device(n, clips, u, w1, r1, g1, k1, w2, r2, g2, k2, o1, o2, ct):
    length, features = u.shape[1:]
    head_count = k1.shape[0]
    size = features // head_count
    heads = head_count // n

    def by_device(g):
        return g.reshape(n, heads, length)

    results = whole(
        n,
        clips,
        size,
        u[0],
        w1[0],
        r1[0],
        by_device(g1),
        k1,
        w2[0],
        r2[0],
        by_device(g2),
        k2,
        o1[None],
        o2[None],
        ct[0],
    )
    factor = 1.0 / math.sqrt(clips * n * length * size)
    du, dw1, dr1, dw2, dr2, dg1, dg2, dk1, dk2 = gather(n, factor, *results)
    return (
        du[None],
        dw1[None],
        dr1[None],
        dg1.reshape(1, head_count, length),
        dk1[0],
        dw2[None],
        dr2[None],
        dg2.reshape(1, head_count, length),
        dk2[0],
    )


def solution(mesh):
    tokens, decay = P("dp", "seq", None), P("dp", None, "seq")
    return jax.shard_map(
        functools.partial(on_device, mesh.shape["seq"], mesh.shape["dp"]),
        mesh=mesh,
        in_specs=(tokens, tokens, tokens, decay, P(), tokens, tokens, decay, P(), P("seq"), P("seq"), tokens),
        out_specs=(tokens, tokens, tokens, decay, P(), tokens, tokens, decay, P()),
        check_vma=False,
    )
```

```python
import functools
import math
import types

import jax
import jax.numpy as jnp
from jax import lax
from jax.experimental import pallas as pl
from jax.experimental.pallas import tpu as pltpu
from jax.sharding import PartitionSpec as P

MESH = pl.DeviceIdType.MESH
HIGHEST = lax.Precision.HIGHEST
F32 = jnp.float32
BF16 = jnp.bfloat16


def nn(a, b, precision=None):
    return lax.dot_general(a, b, (((1,), (0,)), ((), ())), precision=precision, preferred_element_type=F32)


def nt(a, b, precision=None):
    return lax.dot_general(a, b, (((1,), (1,)), ((), ())), precision=precision, preferred_element_type=F32)


def tn(a, b, precision=None):
    return lax.dot_general(a, b, (((0,), (0,)), ((), ())), precision=precision, preferred_element_type=F32)


def iota(shape, dim):
    return lax.broadcasted_iota(jnp.int32, shape, dim)


def two(a):
    high = a.astype(BF16)
    return high, (a - high.astype(F32)).astype(BF16)


def rows_of(*parts):
    return jnp.concatenate(parts, axis=0)


def decay_sums(length):
    half, mid = length // 2, length // 4
    t, s = iota((length + 8, length), 0), iota((length + 8, length), 1)
    first, second = mid, half + mid
    middle = jnp.where(t < half, first, second)
    by_token = (s <= t).astype(F32) - (s < middle).astype(F32)
    k = t - length
    by_chunk = jnp.where(k == 0, (s < first).astype(F32), 0.0)
    by_chunk = jnp.where(k == 1, (s < second).astype(F32), by_chunk)
    by_chunk = jnp.where(k == 2, (s >= first).astype(F32), by_chunk)
    by_chunk = jnp.where(k == 3, (s >= second).astype(F32), by_chunk)
    by_chunk = jnp.where(k == 4, 1.0, by_chunk)
    by_chunk = jnp.where(k == 5, ((s >= first) & (s < second)).astype(F32), by_chunk)
    return jnp.where(k < 0, by_token, by_chunk).astype(BF16)


def factors(log_decay, size):
    heads, length = log_decay.shape
    sums = decay_sums(length)
    wide = [
        jnp.concatenate([jnp.broadcast_to(part[h : h + 1], (size, length)) for h in range(heads)], axis=0).astype(BF16)
        for part in (p.astype(F32) for p in two(log_decay))
    ]
    logs = nt(sums, wide[0]) + nt(sums, wide[1])
    by_token = logs[:length]
    return jnp.exp(by_token), jnp.exp(-by_token), jnp.exp(logs[length:])


def strict_scores(a, b, lower):
    scores = nt(a, b)
    row, col = iota(scores.shape, 0), iota(scores.shape, 1)
    return two(jnp.where(row > col if lower else row < col, scores, 0.0))


def whole_kernel(n, clips, size, factor, held, sems, *refs):
    x = types.SimpleNamespace(**dict(zip(held, refs[21:])))
    x.u, x.w1, x.r1, x.g1, x.k1, x.w2, x.r2, x.g2, x.k2, x.o1, x.o2, x.ct = refs[:12]
    x.dinput, x.dw1, x.dr1, x.dw2, x.dr2, x.decays1_in, x.decays2_in, x.dk1, x.dk2 = refs[12:21]
    x.load, x.rounds = refs[-2:]
    x.__dict__.update(zip(sems, zip(refs[21 + len(held) : -2 : 2], refs[22 + len(held) : -2 : 2])))
    me, clip = lax.axis_index("seq"), lax.axis_index("dp")
    chips = n // 2
    chip, core = lax.div(me, 2), lax.rem(me, 2)
    twin = me + 1 - 2 * core
    heads, length = x.g1.shape[1:]
    features = heads * size
    half = length // 2
    here = pl.ds(pl.multiple_of(me * features, features), features)

    def chunk(b):
        return pl.ds(pl.multiple_of(b * length, length), length)

    def cut(ref, at):
        return ref.at[:, pl.ds(pl.multiple_of(at * features, features), features)]

    barrier = pltpu.get_barrier_semaphore()
    for d in range(1, n):
        pl.semaphore_signal(barrier, inc=1, device_id={"seq": lax.rem(me + d, n)}, device_id_type=MESH)
    lines = ((clip >= 0, clip + 1 - 2 * lax.rem(clip, 2)), (clip >= 2, clip - 2), (clip < clips - 2, clip + 2))
    greetings = sum(jnp.where(there, 1, 0) for there, _ in lines)

    def greet(sem):
        for there, to in lines:

            @pl.when(there)
            def _():
                pl.semaphore_signal(sem, inc=1, device_id={"dp": to}, device_id_type=MESH)

    met = []

    def hear(count):
        for k in range(len(met), count):
            pl.semaphore_wait(x.rounds.at[k], greetings)
            met.append(k)
            if k + 1 < clips // 2 - 1:
                greet(x.rounds.at[k + 1])

    greet(barrier)
    load = pltpu.make_async_copy(x.ct, x.ct_wide, x.load.at[0])
    load.start()
    own_load = pltpu.make_async_copy(cut(x.u, me), x.u_all.at[me], x.load.at[1])
    own_load.start()
    load.wait()
    x.ct_out[...] = x.ct_wide[...].astype(BF16)
    pl.semaphore_wait(barrier, n - 1 + greetings)
    greet(x.rounds.at[0])

    def copy_to(axis, to, src, dst, pair, *at):
        return pltpu.make_async_remote_copy(
            src_ref=src,
            dst_ref=dst,
            send_sem=pair[0].at[at],
            recv_sem=pair[1].at[at],
            device_id={axis: to},
            device_id_type=MESH,
        )

    def device(away, other):
        return 2 * lax.rem(chip + away, chips) + (1 - core if other else core)

    peers = [(away, other) for away in range(1, chips) for other in (0, 1)] + [(0, 1)]
    moves = [
        lambda to: (x.g2.at[to], x.g_all.at[1, me]),
        lambda to: (x.g1.at[to], x.g_all.at[0, me]),
        lambda to: (x.o1, x.o1_all.at[me]),
        lambda to: (x.o2, x.o2_all.at[me]),
    ]
    step = min(2 * length, features)
    tiles = [slice(at, at + step) for at in range(0, features, step)]

    def tile_moves(lanes):
        def at(to):
            return pl.ds(pl.multiple_of(to * features + lanes.start, step), step)

        return [
            lambda to: (x.ct_out.at[:, at(to)], x.ct_all.at[chunk(me), lanes]),
            lambda to: (x.u.at[:, at(to)], x.u_all.at[me, :, lanes]),
        ]

    ct_at = len(moves)
    u_at = ct_at + 1
    for lanes in tiles:
        moves += tile_moves(lanes)
    arriving = [[] for _ in moves]

    def issue(k):
        for away, other in peers:
            to = device(away, other)
            copy = copy_to("seq", to, *moves[k](to), x.move, 2 * away + other - 1, k)
            copy.start()
            arriving[k].append(copy)

    pairs = ((x.w2, x.w_all.at[1]), (x.r2, x.r_all.at[1]), (x.w1, x.w_all.at[0]), (x.r1, x.r_all.at[0]))
    far, near = [], []

    def issue_pair(k):
        src, dst = pairs[k]
        for away in range(1, chips):
            copy = copy_to("seq", device(away, 0), src, dst.at[me], x.near, away - 1, k)
            copy.start()
            far.append(copy)
        copy = copy_to("seq", twin, src, dst.at[me], x.near, chips - 1, k)
        copy.start()
        near.append(copy)

    def wait_for(k):
        for copy in arriving[k]:
            copy.wait_recv()

    issue_pair(0)
    issue_pair(1)
    issue(0)
    issue(1)
    issue_pair(2)
    issue_pair(3)
    for k in range(2, len(moves)):
        issue(k)
    x.g_all[0, me] = x.g1[me]
    x.g_all[1, me] = x.g2[me]
    for src, dst in pairs + ((x.o1, x.o1_all), (x.o2, x.o2_all)):
        dst[me] = src[...]
    x.ct_all[chunk(me)] = x.ct_out[:, here]

    first = me * heads

    def gains(ref):
        channel = iota((1, features), 1) // size
        row = jnp.zeros((1, features), F32)
        for h in range(heads):
            row = jnp.where(channel == h, ref[first + h], row)
        return row

    skips = (gains(x.k1), gains(x.k2))

    def prepare_decays(layer):
        def step(b, carry):
            grown, shrunk, sums = factors(x.g_all[layer, b], size)
            x.grown[layer, b] = grown
            x.shrunk[layer, b] = shrunk
            x.sums[layer, b] = sums
            return carry

        lax.fori_loop(0, n, step, 0, unroll=4)

    def prepare_scores(layer):
        def step(b, carry):
            w, r = x.w_all[layer, b], x.r_all[layer, b]
            x.fore[layer, b], x.fore_low[layer, b] = strict_scores(r, w, True)
            x.back[layer, b], x.back_low[layer, b] = strict_scores(w, r, False)
            return carry

        lax.fori_loop(0, n, step, 0, unroll=4)

    def prepare_order(src, dst, out):
        def step(i, carry):
            cell = jnp.transpose(jnp.broadcast_to(dst[i].astype(F32), (length, length)))
            out[i] = jnp.concatenate([(cell == src[j].astype(F32)).astype(BF16) for j in range(n)], axis=1)
            return carry

        lax.fori_loop(0, n, step, 0, unroll=4)

    wait_for(0)
    hear(1)
    prepare_decays(1)
    wait_for(1)
    prepare_decays(0)
    for copy in far:
        copy.wait_recv()
    for k, (src, dst) in enumerate(pairs):
        for away in range(1, chips):
            block = 2 * lax.rem(chip - away + chips, chips) + core
            copy = copy_to("seq", twin, dst.at[block], dst.at[block], x.near, chips - 1 + away, k)
            copy.start()
            near.append(copy)
    wait_for(2)
    wait_for(3)
    prepare_order(x.o2_all, x.o1_all, x.take_first)
    prepare_order(x.o1_all, x.o2_all, x.take_second)
    for copy in near:
        copy.wait_recv()
    prepare_scores(1)
    prepare_scores(0)
    state, adjoint = x.state, x.adjoint
    adjoint[...] = jnp.zeros_like(adjoint)
    state[...] = jnp.zeros_like(state)

    def own(w, r):
        return jnp.sum(w.astype(F32) * r.astype(F32), axis=1, keepdims=True)

    def back(layer, b, lanes, dy):
        w, r = x.w_all[layer, b], x.r_all[layer, b]
        scores, low = x.back[layer, b], x.back_low[layer, b]
        left_a = jnp.concatenate([w[:half], scores[:half]], axis=1)
        left_z = jnp.concatenate([w[half:], scores[half:]], axis=1)
        wide, sums = dy.astype(F32), x.sums[layer, b, :, lanes]
        scaled = wide * x.grown[layer, b, :, lanes]
        high = scaled.astype(BF16)
        a, z = high[:half], high[half:]
        x.dys[layer, b, :, lanes] = high
        turned = (scaled[half:] * sums[5:6]).astype(BF16)
        end = adjoint[:, lanes]
        carried = rows_of(scaled[:half] * sums[0:1], scaled[half:] * sums[1:2]).astype(BF16)
        adjoint[:, lanes] = end * sums[4:5] + tn(r, carried)
        end_a, end_z = (end * sums[2:3]).astype(BF16), (end * sums[3:4]).astype(BF16)
        x.ends[layer, b, :, lanes] = end
        x.ends_a[layer, b, :, lanes] = end_a
        x.ends_z[layer, b, :, lanes] = end_z
        top = nn(left_a, rows_of(end_a, a, turned)) + nn(low[:half], rows_of(a, turned))
        bottom = nn(left_z, rows_of(end_z, a, z)) + nn(low[half:], high)
        inner = rows_of(top, bottom) * x.shrunk[layer, b, :, lanes]
        x.inner[layer, b, :, lanes] = inner
        return (inner + (skips[layer][:, lanes] + own(w, r)) * wide).astype(BF16)

    lower = iota((length, length), 0) >= iota((length, length), 1)
    since = lower.astype(BF16)
    picks = (iota((features, heads), 0) // size == iota((features, heads), 1)).astype(BF16)

    def forward(layer, b, lanes, u, put):
        w, r = x.w_all[layer, b], x.r_all[layer, b]
        scores, low = x.fore[layer, b], x.fore_low[layer, b]
        left_a = jnp.concatenate([r[:half], scores[:half]], axis=1)
        left_z = jnp.concatenate([r[half:], scores[half:]], axis=1)
        wide, sums = u.astype(F32), x.sums[layer, b, :, lanes]
        scaled = wide * x.shrunk[layer, b, :, lanes]
        high, rest = two(scaled)
        turned, turned_low = two(scaled[:half] * sums[5:6])
        start = state[:, lanes]
        carried, carried_low = two(rows_of(scaled[:half] * sums[2:3], scaled[half:] * sums[3:4]))
        after = start * sums[4:5] + tn(w, carried)
        if put:
            after = after + tn(w, carried_low)
        state[:, lanes] = after
        start_a, start_a_low = two(start * sums[0:1])
        start_z, start_z_low = two(start * sums[1:2])
        other, other_low = rows_of(turned, high[half:]), rows_of(turned_low, rest[half:])
        top = nn(left_a, rows_of(start_a, high))
        bottom = nn(left_z, rows_of(start_z, other))
        if put:
            top = top + nn(low[:half], high) + nn(left_a, rows_of(start_a_low, rest))
            bottom = bottom + nn(low[half:], other) + nn(left_z, rows_of(start_z_low, other_low))
        inner = rows_of(top, bottom) * x.grown[layer, b, :, lanes]
        if put:
            put(wide, (inner + (skips[layer][:, lanes] + own(w, r)) * wide).astype(BF16))
        x.us[layer, b, 0, :, lanes] = high
        if put:
            x.us[layer, b, 1, :, lanes] = rest
            x.turns[layer, b, 1, :, lanes] = turned_low
        x.turns[layer, b, 0, :, lanes] = turned
        x.starts_a[layer, b, :, lanes] = start_a
        x.starts_z[layer, b, :, lanes] = start_z
        x.through[layer, b, :, lanes] = jnp.sum(x.ends[layer, b, :, lanes] * after, axis=0, keepdims=True)
        x.outer[layer, b, :, lanes] = inner

    kept = (x.kept_heads, x.kept_scores, x.kept_reads, x.kept_writes)

    def grads(layer, b, tile, u, dy):
        w, r, lanes = x.w_all[layer, b], x.r_all[layer, b], tiles[tile]
        wide, wide_dy = u.astype(F32), dy.astype(F32)
        terms = wide_dy * x.outer[layer, b, :, lanes] - wide * x.inner[layer, b, :, lanes]
        through = jnp.where(iota((8, step), 0) == 7, x.through[layer, b, :, lanes], 0.0)
        terms, terms_low = two(rows_of(terms[: length - 8], terms[length - 8 :] + through))
        high = x.us[layer, b, 0, :, lanes]
        other = rows_of(x.turns[layer, b, 0, :, lanes], high[half:])
        dys = x.dys[layer, b, :, lanes]
        dy_a, dy_z = dys[:half], dys[half:]
        dscores = rows_of(nt(dy_a, high), nt(dy_z, other))
        if layer == 0:
            rest = x.us[layer, b, 1, :, lanes]
            other_low = rows_of(x.turns[layer, b, 1, :, lanes], rest[half:])
            dscores = dscores + rows_of(nt(dy_a, rest), nt(dy_z, other_low))
        totals = (
            nn(terms, picks[lanes]) + nn(terms_low, picks[lanes]),
            dscores,
            rows_of(nt(dy_a, x.starts_a[layer, b, :, lanes]), nt(dy_z, x.starts_z[layer, b, :, lanes])),
            rows_of(nt(high[:half], x.ends_a[layer, b, :, lanes]), nt(high[half:], x.ends_z[layer, b, :, lanes])),
        )
        totals = (totals[0], jnp.where(lower, totals[1], 0.0)) + totals[2:]
        if tile:
            totals = tuple(part + ref[layer, b] for part, ref in zip(totals, kept))
        if tile < len(tiles) - 1:
            for part, ref in zip(totals, kept):
                ref[layer, b] = part
            return
        by_head, by_head_low = two(totals[0])
        x.decays[layer, b] = tn(by_head, since) + tn(by_head_low, since)
        dscores, dscores_low = two(totals[1])
        x.params[layer, b, 0] = tn(dscores, r) + tn(dscores_low, r) + totals[3]
        x.params[layer, b, 1] = nn(dscores, w) + nn(dscores_low, w) + totals[2]

    decays_in = (x.decays1_in, x.decays2_in)

    def input_copy(to, tile, slot):
        at = pl.ds(pl.multiple_of(me * features + tiles[tile].start, step), step)
        return copy_to("seq", to, x.du1.at[to, :, tiles[tile]], x.dinput.at[:, at], x.input, tile, slot)

    def decay_copy(layer, to, slot):
        return copy_to("seq", to, x.decays.at[layer, to], decays_in[layer].at[me], x.decay, layer, slot)

    def twin_copy(layer, owner, slot):
        return copy_to("seq", twin, x.params.at[layer, owner], x.twins.at[layer, slot], x.twin, layer, slot)

    def leave(layer):
        for d in range(1, n):
            decay_copy(layer, lax.rem(me + d, n), d - 1).start()
        for away in range(chips):
            twin_copy(layer, device(away, 1), away).start()

    chip_copies = []

    def leave_chip(layer):
        for away in range(1, chips):
            owner = device(away, 0)
            twin_copy(layer, device(away, 1), away).wait_recv()
            total = x.params[layer, owner] + x.twins[layer, away]
            x.chip_sums[layer, away] = total.astype(BF16)
            copy = copy_to(
                "seq", owner, x.chip_sums.at[layer, away], x.chips_in.at[layer, away], x.chip, layer, away
            )
            copy.start()
            chip_copies.append(copy)

    hear(2)
    own_load.wait()
    x.skips[...] = jnp.zeros_like(x.skips)
    clip_copies = []

    def send_skips():
        channel, head = iota((features, length), 0) // size, iota((features, length), 1)
        x.by_head[...] = nn(x.skips[...], (channel == head).astype(F32), HIGHEST) * factor
        for d in range(1, clips):
            to = lax.rem(clip + d, clips)
            copy = copy_to("dp", to, x.by_head, x.clips_in.at[clip], x.clip, d - 1)
            copy.start()
            clip_copies.append(copy)
        x.clips_in[clip] = x.by_head[...]

    def pass_tile(tile):
        lanes, final = tiles[tile], tile == len(tiles) - 1

        wait_for(ct_at + 2 * tile)

        def back_second(i, carry):
            b = n - 1 - i
            x.du2[chunk(b), lanes] = back(1, b, lanes, x.ct_all[chunk(b), lanes])
            return carry

        lax.fori_loop(0, n, back_second, 0, unroll=4)

        def regrid_back(i, carry):
            x.dy1[chunk(i), lanes] = nn(x.take_first[i], x.du2[:, lanes]).astype(BF16)
            x.ct_first[chunk(i), lanes] = nn(x.take_first[i], x.ct_all[:, lanes]).astype(BF16)
            return carry

        lax.fori_loop(0, n, regrid_back, 0, unroll=4)
        adjoint[:, lanes] = jnp.zeros((adjoint.shape[0], step), F32)

        def back_first(i, carry):
            b = n - 1 - i
            x.du1[b, :, lanes] = back(0, b, lanes, x.dy1[chunk(b), lanes])
            return carry

        lax.fori_loop(0, n, back_first, 0, unroll=4)
        for d in range(1, n):
            input_copy(lax.rem(me + d, n), tile, d - 1).start()
        wait_for(u_at + 2 * tile)

        def first_layer(b, carry):
            def put(wide, value):
                x.y1[chunk(b), lanes] = value
                x.skips[0:1, lanes] += jnp.sum(wide * x.dy1[chunk(b), lanes].astype(F32), axis=0, keepdims=True)
                upstream = x.ct_first[chunk(b), lanes].astype(F32)
                x.skips[1:2, lanes] += jnp.sum(value.astype(F32) * upstream, axis=0, keepdims=True)

            forward(0, b, lanes, x.u_all[b, :, lanes], put)
            return carry

        lax.fori_loop(0, n, first_layer, 0, unroll=4)
        if final:
            hear(clips // 2 - 1)
            send_skips()

        def regrid(i, carry):
            x.u2[i, :, lanes] = nn(x.take_second[i], x.y1[:, lanes]).astype(BF16)
            return carry

        lax.fori_loop(0, n, regrid, 0, unroll=4)
        state[:, lanes] = jnp.zeros((state.shape[0], step), F32)

        def second_layer(b, carry):
            forward(1, b, lanes, x.u2[b, :, lanes], None)
            grads(0, b, tile, x.u_all[b, :, lanes], x.dy1[chunk(b), lanes])
            return carry

        lax.fori_loop(0, n, second_layer, 0, unroll=4)
        if final:
            leave(0)

        def second_grads(b, carry):
            grads(1, b, tile, x.u2[b, :, lanes], x.ct_all[chunk(b), lanes])
            return carry

        lax.fori_loop(0, n, second_grads, 0, unroll=4)
        if final:
            leave(1)
            leave_chip(0)
            leave_chip(1)

    for tile in range(len(tiles)):
        pass_tile(tile)
    for copy in clip_copies:
        copy.wait()
    x.summed[...] = jnp.sum(x.clips_in[...], axis=0)
    last = []
    for d in range(1, n):
        to = lax.rem(me + d, n)
        copy = copy_to("seq", to, x.summed, x.parts_in.at[me], x.part, d - 1)
        copy.start()
        last.append(copy)
    x.parts_in[me] = x.summed[...]
    own_input = pltpu.make_async_copy(x.du1.at[me], cut(x.dinput, me), x.load.at[0])
    own_input.start()
    for layer in range(2):
        decays_in[layer][me] = x.decays[layer, me]
    for layer, outs in enumerate(((x.dw1, x.dr1), (x.dw2, x.dr2))):
        twin_copy(layer, twin, 0).wait_recv()
        for k, out in enumerate(outs):
            total = x.params[layer, me, k] + x.twins[layer, 0, k]
            if k == 0:
                for copy in chip_copies[layer * (chips - 1) : (layer + 1) * (chips - 1)]:
                    copy.wait_recv()
            for away in range(1, chips):
                total = total + x.chips_in[layer, away, k].astype(F32)
            out[...] = total.astype(BF16)
    for group in arriving:
        for copy in group:
            copy.wait_send()
    for copy in far + near + chip_copies:
        copy.wait_send()
    for layer in range(2):
        for away in range(chips):
            twin_copy(layer, device(away, 1), away).wait_send()
    for d in range(1, n):
        to = lax.rem(me + d, n)
        last += [input_copy(to, tile, d - 1) for tile in range(len(tiles))]
        last += [decay_copy(0, to, d - 1), decay_copy(1, to, d - 1)]
    for copy in last:
        copy.wait()
    for s in range(n):
        for k, out in enumerate((x.dk1, x.dk2)):
            out[:, s * heads : (s + 1) * heads] = x.parts_in[s, k : k + 1, :heads]
    own_input.wait()


def whole(n, clips, size, factor, *args):
    length, width = args[0].shape
    heads = args[3].shape[1]
    count = args[1].shape[1]
    features, half, chips = heads * size, length // 2, n // 2
    vmem = pl.BlockSpec(memory_space=pltpu.VMEM)
    smem = pl.BlockSpec(memory_space=pltpu.SMEM)
    away = pl.BlockSpec(memory_space=pl.ANY)
    param, decay, gain = (length, count), (n, heads, length), (2, features)
    wide, flat, held, square = (n, length, features), (n * length, features), (n, count, features), (n, length, length)
    order, pick, pair = (n, 1, length), (n, length, n * length), (2, length, count)
    outs = (((length, width), BF16),) + ((param, BF16),) * 4 + ((decay, F32),) * 2 + (((1, n * heads), F32),) * 2
    scratch = dict(
        ct_out=((length, width), BF16),
        ct_wide=((length, width), F32),
        u_all=(wide, BF16),
        ct_all=(flat, BF16),
        ct_first=(flat, BF16),
        w_all=((2, n) + param, BF16),
        r_all=((2, n) + param, BF16),
        g_all=((2,) + decay, F32),
        o1_all=(order, jnp.int32),
        o2_all=(order, jnp.int32),
        grown=((2,) + wide, F32),
        shrunk=((2,) + wide, F32),
        sums=((2, n, 8, features), F32),
        fore=((2,) + square, BF16),
        fore_low=((2,) + square, BF16),
        back=((2,) + square, BF16),
        back_low=((2,) + square, BF16),
        take_first=(pick, BF16),
        take_second=(pick, BF16),
        du2=(flat, BF16),
        dy1=(flat, BF16),
        y1=(flat, BF16),
        u2=(wide, BF16),
        du1=(wide, BF16),
        dys=((2,) + wide, BF16),
        ends=((2,) + held, F32),
        ends_a=((2,) + held, BF16),
        ends_z=((2,) + held, BF16),
        inner=((2,) + wide, F32),
        outer=((2,) + wide, F32),
        us=((2, n, 2, length, features), BF16),
        turns=((2, n, 2, half, features), BF16),
        starts_a=((2,) + held, BF16),
        starts_z=((2,) + held, BF16),
        through=((2, n, 1, features), F32),
        kept_heads=((2, n, length, heads), F32),
        kept_scores=((2,) + square, F32),
        kept_reads=((2, n) + param, F32),
        kept_writes=((2, n) + param, F32),
        state=((count, features), F32),
        adjoint=((count, features), F32),
        params=((2, n) + pair, F32),
        twins=((2, chips) + pair, F32),
        chip_sums=((2, chips) + pair, BF16),
        chips_in=((2, chips) + pair, BF16),
        decays=((2,) + decay, F32),
        skips=(gain, F32),
        by_head=((2, length), F32),
        clips_in=((clips, 2, length), F32),
        summed=((2, length), F32),
        parts_in=((n, 2, length), F32),
    )
    sems = dict(
        move=(n - 1, 4 + 2 * max(1, features // (2 * length))),
        near=(n - 1, 4),
        input=(max(1, features // (2 * length)), n - 1),
        decay=(2, n - 1),
        twin=(2, chips),
        chip=(2, chips),
        clip=(clips - 1,),
        part=(n - 1,),
    )
    taken = sum(math.prod(shape) * jnp.dtype(kind).itemsize for shape, kind in scratch.values())
    return pl.pallas_call(
        functools.partial(whole_kernel, n, clips, size, factor, tuple(scratch), tuple(sems)),
        out_shape=tuple(jax.ShapeDtypeStruct(*out) for out in outs),
        in_specs=[away] + [vmem] * 3 + [smem] + [vmem] * 3 + [smem] + [vmem] * 2 + [away],
        out_specs=[away] + [vmem] * 8,
        scratch_shapes=[pltpu.VMEM(*one) for one in scratch.values()]
        + [pltpu.SemaphoreType.DMA(shape) for shape in sems.values() for _ in range(2)]
        + [pltpu.SemaphoreType.DMA((2,)), pltpu.SemaphoreType.REGULAR((clips // 2 - 1,))],
        compiler_params=pltpu.CompilerParams(
            collective_id=0, has_side_effects=True
        ),
        name="whole",
    )(*args)


def gather_kernel(count, *refs):
    sources, results, held, sems = refs[:count], refs[count : 2 * count], refs[2 * count : 3 * count], refs[-2:]
    pieces = []
    for k, source in enumerate(sources):
        step = max(source.shape[0] // 4, 1) if k == 0 else source.shape[0]
        pieces += [(k, pl.ds(at, step)) for at in range(0, source.shape[0], step)]
    loads, stores = [], []
    for at, (k, rows) in enumerate(pieces):
        loads.append(pltpu.make_async_copy(sources[k].at[rows], held[k].at[rows], sems[0].at[at]))
        stores.append(pltpu.make_async_copy(held[k].at[rows], results[k].at[rows], sems[1].at[at]))
        loads[-1].start()
    for load, store in zip(loads, stores):
        load.wait()
        store.start()
    for store in stores:
        store.wait()


def gather(*results):
    away = pl.BlockSpec(memory_space=pl.ANY)
    count = len(results)
    return pl.pallas_call(
        functools.partial(gather_kernel, count),
        out_shape=tuple(jax.ShapeDtypeStruct(one.shape, one.dtype) for one in results),
        in_specs=[away] * count,
        out_specs=[away] * count,
        scratch_shapes=[pltpu.VMEM(one.shape, one.dtype) for one in results]
        + [pltpu.SemaphoreType.DMA((count + 3,))] * 2,
        name="gather",
    )(*results)


def on_device(n, clips, u, w1, r1, g1, k1, w2, r2, g2, k2, o1, o2, ct):
    length, features = u.shape[1:]
    head_count = k1.shape[0]
    size = features // head_count
    heads = head_count // n

    def by_device(g):
        return g.reshape(n, heads, length)

    results = whole(
        n,
        clips,
        size,
        1.0 / math.sqrt(clips * n * length * size),
        u[0],
        w1[0],
        r1[0],
        by_device(g1),
        k1,
        w2[0],
        r2[0],
        by_device(g2),
        k2,
        o1[None],
        o2[None],
        ct[0],
    )
    du, dw1, dr1, dw2, dr2, dg1, dg2, dk1, dk2 = gather(*results)
    return (
        du[None],
        dw1[None],
        dr1[None],
        dg1.reshape(1, head_count, length),
        dk1[0],
        dw2[None],
        dr2[None],
        dg2.reshape(1, head_count, length),
        dk2[0],
    )


def solution(mesh):
    tokens, decay = P("dp", "seq", None), P("dp", None, "seq")
    return jax.shard_map(
        functools.partial(on_device, mesh.shape["seq"], mesh.shape["dp"]),
        mesh=mesh,
        in_specs=(tokens, tokens, tokens, decay, P(), tokens, tokens, decay, P(), P("seq"), P("seq"), tokens),
        out_specs=(tokens, tokens, tokens, decay, P(), tokens, tokens, decay, P()),
        check_vma=False,
    )
```

```python
import functools
import math
import types

import jax
import jax.numpy as jnp
from jax import lax
from jax.experimental import pallas as pl
from jax.experimental.pallas import tpu as pltpu
from jax.sharding import PartitionSpec as P

MESH = pl.DeviceIdType.MESH
HIGHEST = lax.Precision.HIGHEST
F32 = jnp.float32
BF16 = jnp.bfloat16


def nn(a, b, precision=None):
    return lax.dot_general(a, b, (((1,), (0,)), ((), ())), precision=precision, preferred_element_type=F32)


def nt(a, b, precision=None):
    return lax.dot_general(a, b, (((1,), (1,)), ((), ())), precision=precision, preferred_element_type=F32)


def tn(a, b, precision=None):
    return lax.dot_general(a, b, (((0,), (0,)), ((), ())), precision=precision, preferred_element_type=F32)


def iota(shape, dim):
    return lax.broadcasted_iota(jnp.int32, shape, dim)


def two(a):
    high = a.astype(BF16)
    return high, (a - high.astype(F32)).astype(BF16)


def rows_of(*parts):
    return jnp.concatenate(parts, axis=0)


def decay_sums(length):
    half, mid = length // 2, length // 4
    t, s = iota((length + 8, length), 0), iota((length + 8, length), 1)
    first, second = mid, half + mid
    middle = jnp.where(t < half, first, second)
    by_token = (s <= t).astype(F32) - (s < middle).astype(F32)
    k = t - length
    by_chunk = jnp.where(k == 0, (s < first).astype(F32), 0.0)
    by_chunk = jnp.where(k == 1, (s < second).astype(F32), by_chunk)
    by_chunk = jnp.where(k == 2, (s >= first).astype(F32), by_chunk)
    by_chunk = jnp.where(k == 3, (s >= second).astype(F32), by_chunk)
    by_chunk = jnp.where(k == 4, 1.0, by_chunk)
    by_chunk = jnp.where(k == 5, ((s >= first) & (s < second)).astype(F32), by_chunk)
    return jnp.where(k < 0, by_token, by_chunk).astype(BF16)


def factors(log_decay, size):
    heads, length = log_decay.shape
    sums = decay_sums(length)
    wide = [
        jnp.concatenate([jnp.broadcast_to(part[h : h + 1], (size, length)) for h in range(heads)], axis=0).astype(BF16)
        for part in (p.astype(F32) for p in two(log_decay))
    ]
    logs = nt(sums, wide[0]) + nt(sums, wide[1])
    by_token = logs[:length]
    return jnp.exp(by_token), jnp.exp(-by_token), jnp.exp(logs[length:])


def strict_scores(a, b, lower):
    scores = nt(a, b)
    row, col = iota(scores.shape, 0), iota(scores.shape, 1)
    return two(jnp.where(row > col if lower else row < col, scores, 0.0))


def whole_kernel(n, clips, size, factor, held, sems, *refs):
    x = types.SimpleNamespace(**dict(zip(held, refs[21:])))
    x.u, x.w1, x.r1, x.g1, x.k1, x.w2, x.r2, x.g2, x.k2, x.o1, x.o2, x.ct = refs[:12]
    x.dinput, x.dw1, x.dr1, x.dw2, x.dr2, x.decays1_in, x.decays2_in, x.dk1, x.dk2 = refs[12:21]
    x.load, x.rounds = refs[-2:]
    x.__dict__.update(zip(sems, zip(refs[21 + len(held) : -2 : 2], refs[22 + len(held) : -2 : 2])))
    me, clip = lax.axis_index("seq"), lax.axis_index("dp")
    chips = n // 2
    chip, core = lax.div(me, 2), lax.rem(me, 2)
    twin = me + 1 - 2 * core
    heads, length = x.g1.shape[1:]
    features = heads * size
    half = length // 2
    here = pl.ds(pl.multiple_of(me * features, features), features)

    def chunk(b):
        return pl.ds(pl.multiple_of(b * length, length), length)

    def cut(ref, at):
        return ref.at[:, pl.ds(pl.multiple_of(at * features, features), features)]

    barrier = pltpu.get_barrier_semaphore()
    for d in range(1, n):
        pl.semaphore_signal(barrier, inc=1, device_id={"seq": lax.rem(me + d, n)}, device_id_type=MESH)
    lines = ((clip >= 0, clip + 1 - 2 * lax.rem(clip, 2)), (clip >= 2, clip - 2), (clip < clips - 2, clip + 2))
    greetings = sum(jnp.where(there, 1, 0) for there, _ in lines)

    def greet(sem):
        for there, to in lines:

            @pl.when(there)
            def _():
                pl.semaphore_signal(sem, inc=1, device_id={"dp": to}, device_id_type=MESH)

    met = []

    def hear(count):
        for k in range(len(met), count):
            pl.semaphore_wait(x.rounds.at[k], greetings)
            met.append(k)
            if k + 1 < clips // 2 - 1:
                greet(x.rounds.at[k + 1])

    greet(barrier)
    load = pltpu.make_async_copy(x.ct, x.ct_wide, x.load.at[0])
    load.start()
    own_load = pltpu.make_async_copy(cut(x.u, me), x.u_all.at[me], x.load.at[1])
    own_load.start()
    load.wait()
    x.ct_out[...] = x.ct_wide[...].astype(BF16)
    pl.semaphore_wait(barrier, n - 1 + greetings)
    greet(x.rounds.at[0])

    def copy_to(axis, to, src, dst, pair, *at):
        return pltpu.make_async_remote_copy(
            src_ref=src,
            dst_ref=dst,
            send_sem=pair[0].at[at],
            recv_sem=pair[1].at[at],
            device_id={axis: to},
            device_id_type=MESH,
        )

    def device(away, other):
        return 2 * lax.rem(chip + away, chips) + (1 - core if other else core)

    peers = [(away, other) for away in range(1, chips) for other in (0, 1)] + [(0, 1)]
    moves = [
        lambda to: (x.g2.at[to], x.g_all.at[1, me]),
        lambda to: (x.g1.at[to], x.g_all.at[0, me]),
        lambda to: (x.o1, x.o1_all.at[me]),
        lambda to: (x.o2, x.o2_all.at[me]),
    ]
    step = min(2 * length, features)
    tiles = [slice(at, at + step) for at in range(0, features, step)]

    def tile_moves(lanes):
        def at(to):
            return pl.ds(pl.multiple_of(to * features + lanes.start, step), step)

        return [
            lambda to: (x.ct_out.at[:, at(to)], x.ct_all.at[chunk(me), lanes]),
            lambda to: (x.u.at[:, at(to)], x.u_all.at[me, :, lanes]),
        ]

    ct_at = len(moves)
    u_at = ct_at + 1
    for lanes in tiles:
        moves += tile_moves(lanes)
    arriving = [[] for _ in moves]

    def issue(k):
        for away, other in peers:
            to = device(away, other)
            copy = copy_to("seq", to, *moves[k](to), x.move, 2 * away + other - 1, k)
            copy.start()
            arriving[k].append(copy)

    pairs = ((x.w2, x.w_all.at[1]), (x.r2, x.r_all.at[1]), (x.w1, x.w_all.at[0]), (x.r1, x.r_all.at[0]))
    far, near = [], []

    def issue_pair(k):
        src, dst = pairs[k]
        for away in range(1, chips):
            copy = copy_to("seq", device(away, 0), src, dst.at[me], x.near, away - 1, k)
            copy.start()
            far.append(copy)
        copy = copy_to("seq", twin, src, dst.at[me], x.near, chips - 1, k)
        copy.start()
        near.append(copy)

    def wait_for(k):
        for copy in arriving[k]:
            copy.wait_recv()

    issue_pair(0)
    issue_pair(1)
    issue(0)
    issue(1)
    issue_pair(2)
    issue_pair(3)
    for k in range(2, len(moves)):
        issue(k)
    x.g_all[0, me] = x.g1[me]
    x.g_all[1, me] = x.g2[me]
    for src, dst in pairs + ((x.o1, x.o1_all), (x.o2, x.o2_all)):
        dst[me] = src[...]
    x.ct_all[chunk(me)] = x.ct_out[:, here]

    first = me * heads

    def gains(ref):
        channel = iota((1, features), 1) // size
        row = jnp.zeros((1, features), F32)
        for h in range(heads):
            row = jnp.where(channel == h, ref[first + h], row)
        return row

    skips = (gains(x.k1), gains(x.k2))

    def prepare_decays(layer):
        def step(b, carry):
            grown, shrunk, sums = factors(x.g_all[layer, b], size)
            x.grown[layer, b] = grown
            x.shrunk[layer, b] = shrunk
            x.sums[layer, b] = sums
            return carry

        lax.fori_loop(0, n, step, 0, unroll=4)

    def prepare_scores(layer):
        def step(b, carry):
            w, r = x.w_all[layer, b], x.r_all[layer, b]
            x.fore[layer, b], x.fore_low[layer, b] = strict_scores(r, w, True)
            x.back[layer, b], x.back_low[layer, b] = strict_scores(w, r, False)
            return carry

        lax.fori_loop(0, n, step, 0, unroll=4)

    def prepare_order(src, dst, out):
        def step(i, carry):
            cell = jnp.transpose(jnp.broadcast_to(dst[i].astype(F32), (length, length)))
            out[i] = jnp.concatenate([(cell == src[j].astype(F32)).astype(BF16) for j in range(n)], axis=1)
            return carry

        lax.fori_loop(0, n, step, 0, unroll=4)

    wait_for(0)
    hear(1)
    prepare_decays(1)
    wait_for(1)
    prepare_decays(0)
    for copy in far:
        copy.wait_recv()
    for k, (src, dst) in enumerate(pairs):
        for away in range(1, chips):
            block = 2 * lax.rem(chip - away + chips, chips) + core
            copy = copy_to("seq", twin, dst.at[block], dst.at[block], x.near, chips - 1 + away, k)
            copy.start()
            near.append(copy)
    wait_for(2)
    wait_for(3)
    prepare_order(x.o2_all, x.o1_all, x.take_first)
    prepare_order(x.o1_all, x.o2_all, x.take_second)
    for copy in near:
        copy.wait_recv()
    prepare_scores(1)
    prepare_scores(0)
    state, adjoint = x.state, x.adjoint
    adjoint[...] = jnp.zeros_like(adjoint)
    state[...] = jnp.zeros_like(state)

    def own(w, r):
        return jnp.sum(w.astype(F32) * r.astype(F32), axis=1, keepdims=True)

    def back(layer, b, lanes, dy):
        w, r = x.w_all[layer, b], x.r_all[layer, b]
        scores, low = x.back[layer, b], x.back_low[layer, b]
        left_a = jnp.concatenate([w[:half], scores[:half]], axis=1)
        left_z = jnp.concatenate([w[half:], scores[half:]], axis=1)
        wide, sums = dy.astype(F32), x.sums[layer, b, :, lanes]
        scaled = wide * x.grown[layer, b, :, lanes]
        high = scaled.astype(BF16)
        a, z = high[:half], high[half:]
        x.dys[layer, b, :, lanes] = high
        turned = (scaled[half:] * sums[5:6]).astype(BF16)
        end = adjoint[:, lanes]
        carried = rows_of(scaled[:half] * sums[0:1], scaled[half:] * sums[1:2]).astype(BF16)
        adjoint[:, lanes] = end * sums[4:5] + tn(r, carried)
        end_a, end_z = (end * sums[2:3]).astype(BF16), (end * sums[3:4]).astype(BF16)
        x.ends[layer, b, :, lanes] = end
        x.ends_a[layer, b, :, lanes] = end_a
        x.ends_z[layer, b, :, lanes] = end_z
        top = nn(left_a, rows_of(end_a, a, turned)) + nn(low[:half], rows_of(a, turned))
        bottom = nn(left_z, rows_of(end_z, a, z)) + nn(low[half:], high)
        inner = rows_of(top, bottom) * x.shrunk[layer, b, :, lanes]
        x.inner[layer, b, :, lanes] = inner
        return (inner + (skips[layer][:, lanes] + own(w, r)) * wide).astype(BF16)

    lower = iota((length, length), 0) >= iota((length, length), 1)
    since = lower.astype(BF16)
    picks = (iota((features, heads), 0) // size == iota((features, heads), 1)).astype(BF16)

    def forward(layer, b, lanes, u, put):
        w, r = x.w_all[layer, b], x.r_all[layer, b]
        scores, low = x.fore[layer, b], x.fore_low[layer, b]
        left_a = jnp.concatenate([r[:half], scores[:half]], axis=1)
        left_z = jnp.concatenate([r[half:], scores[half:]], axis=1)
        wide, sums = u.astype(F32), x.sums[layer, b, :, lanes]
        scaled = wide * x.shrunk[layer, b, :, lanes]
        high, rest = two(scaled)
        turned, turned_low = two(scaled[:half] * sums[5:6])
        start = state[:, lanes]
        carried, carried_low = two(rows_of(scaled[:half] * sums[2:3], scaled[half:] * sums[3:4]))
        after = start * sums[4:5] + tn(w, carried)
        if put:
            after = after + tn(w, carried_low)
        state[:, lanes] = after
        start_a, start_a_low = two(start * sums[0:1])
        start_z, start_z_low = two(start * sums[1:2])
        other, other_low = rows_of(turned, high[half:]), rows_of(turned_low, rest[half:])
        top = nn(left_a, rows_of(start_a, high))
        bottom = nn(left_z, rows_of(start_z, other))
        if put:
            top = top + nn(low[:half], high) + nn(left_a, rows_of(start_a_low, rest))
            bottom = bottom + nn(low[half:], other) + nn(left_z, rows_of(start_z_low, other_low))
        inner = rows_of(top, bottom) * x.grown[layer, b, :, lanes]
        if put:
            put(wide, (inner + (skips[layer][:, lanes] + own(w, r)) * wide).astype(BF16))
        x.us[layer, b, 0, :, lanes] = high
        if put:
            x.us[layer, b, 1, :, lanes] = rest
            x.turns[layer, b, 1, :, lanes] = turned_low
        x.turns[layer, b, 0, :, lanes] = turned
        x.starts_a[layer, b, :, lanes] = start_a
        x.starts_z[layer, b, :, lanes] = start_z
        x.through[layer, b, :, lanes] = jnp.sum(x.ends[layer, b, :, lanes] * after, axis=0, keepdims=True)
        x.outer[layer, b, :, lanes] = inner

    kept = (x.kept_heads, x.kept_scores, x.kept_reads, x.kept_writes)

    def grads(layer, b, tile, u, dy):
        w, r, lanes = x.w_all[layer, b], x.r_all[layer, b], tiles[tile]
        wide, wide_dy = u.astype(F32), dy.astype(F32)
        terms = wide_dy * x.outer[layer, b, :, lanes] - wide * x.inner[layer, b, :, lanes]
        through = jnp.where(iota((8, step), 0) == 7, x.through[layer, b, :, lanes], 0.0)
        terms, terms_low = two(rows_of(terms[: length - 8], terms[length - 8 :] + through))
        high = x.us[layer, b, 0, :, lanes]
        other = rows_of(x.turns[layer, b, 0, :, lanes], high[half:])
        dys = x.dys[layer, b, :, lanes]
        dy_a, dy_z = dys[:half], dys[half:]
        dscores = rows_of(nt(dy_a, high), nt(dy_z, other))
        if layer == 0:
            rest = x.us[layer, b, 1, :, lanes]
            other_low = rows_of(x.turns[layer, b, 1, :, lanes], rest[half:])
            dscores = dscores + rows_of(nt(dy_a, rest), nt(dy_z, other_low))
        totals = (
            nn(terms, picks[lanes]) + nn(terms_low, picks[lanes]),
            dscores,
            rows_of(nt(dy_a, x.starts_a[layer, b, :, lanes]), nt(dy_z, x.starts_z[layer, b, :, lanes])),
            rows_of(nt(high[:half], x.ends_a[layer, b, :, lanes]), nt(high[half:], x.ends_z[layer, b, :, lanes])),
        )
        totals = (totals[0], jnp.where(lower, totals[1], 0.0)) + totals[2:]
        if tile:
            totals = tuple(part + ref[layer, b] for part, ref in zip(totals, kept))
        if tile < len(tiles) - 1:
            for part, ref in zip(totals, kept):
                ref[layer, b] = part
            return
        by_head, by_head_low = two(totals[0])
        x.decays[layer, b] = tn(by_head, since) + tn(by_head_low, since)
        dscores, dscores_low = two(totals[1])
        x.params[layer, b, 0] = tn(dscores, r) + tn(dscores_low, r) + totals[3]
        x.params[layer, b, 1] = nn(dscores, w) + nn(dscores_low, w) + totals[2]

    decays_in = (x.decays1_in, x.decays2_in)

    def input_copy(to, tile, slot):
        at = pl.ds(pl.multiple_of(me * features + tiles[tile].start, step), step)
        return copy_to("seq", to, x.du1.at[to, :, tiles[tile]], x.dinput.at[:, at], x.input, tile, slot)

    def decay_copy(layer, to, slot):
        return copy_to("seq", to, x.decays.at[layer, to], decays_in[layer].at[me], x.decay, layer, slot)

    def twin_copy(layer, owner, slot):
        return copy_to("seq", twin, x.params.at[layer, owner], x.twins.at[layer, slot], x.twin, layer, slot)

    def leave(layer, ways):
        for away in ways:
            twin_copy(layer, device(away, 1), away).start()

    def leave_decays(layer):
        for d in range(1, n):
            decay_copy(layer, lax.rem(me + d, n), d - 1).start()

    chip_copies = []

    def leave_chip(layer):
        for away in range(1, chips):
            owner = device(away, 0)
            twin_copy(layer, device(away, 1), away).wait_recv()
            total = x.params[layer, owner] + x.twins[layer, away]
            x.chip_sums[layer, away] = total.astype(BF16)
            copy = copy_to(
                "seq", owner, x.chip_sums.at[layer, away], x.chips_in.at[layer, away], x.chip, layer, away
            )
            copy.start()
            chip_copies.append(copy)

    hear(2)
    own_load.wait()
    x.skips[...] = jnp.zeros_like(x.skips)
    clip_copies = []

    def send_skips():
        channel, head = iota((features, length), 0) // size, iota((features, length), 1)
        x.by_head[...] = nn(x.skips[...], (channel == head).astype(F32), HIGHEST) * factor
        for d in range(1, clips):
            to = lax.rem(clip + d, clips)
            copy = copy_to("dp", to, x.by_head, x.clips_in.at[clip], x.clip, d - 1)
            copy.start()
            clip_copies.append(copy)
        x.clips_in[clip] = x.by_head[...]

    def pass_tile(tile):
        lanes, final = tiles[tile], tile == len(tiles) - 1

        wait_for(ct_at + 2 * tile)

        def back_second(i, carry):
            b = n - 1 - i
            x.du2[chunk(b), lanes] = back(1, b, lanes, x.ct_all[chunk(b), lanes])
            return carry

        lax.fori_loop(0, n, back_second, 0, unroll=4)

        def regrid_back(i, carry):
            x.dy1[chunk(i), lanes] = nn(x.take_first[i], x.du2[:, lanes]).astype(BF16)
            x.ct_first[chunk(i), lanes] = nn(x.take_first[i], x.ct_all[:, lanes]).astype(BF16)
            return carry

        lax.fori_loop(0, n, regrid_back, 0, unroll=4)
        adjoint[:, lanes] = jnp.zeros((adjoint.shape[0], step), F32)

        def back_first(i, carry):
            b = n - 1 - i
            x.du1[b, :, lanes] = back(0, b, lanes, x.dy1[chunk(b), lanes])
            return carry

        lax.fori_loop(0, n, back_first, 0, unroll=4)
        for d in range(1, n):
            input_copy(lax.rem(me + d, n), tile, d - 1).start()
        wait_for(u_at + 2 * tile)

        def first_layer(b, carry):
            def put(wide, value):
                x.y1[chunk(b), lanes] = value
                x.skips[0:1, lanes] += jnp.sum(wide * x.dy1[chunk(b), lanes].astype(F32), axis=0, keepdims=True)
                upstream = x.ct_first[chunk(b), lanes].astype(F32)
                x.skips[1:2, lanes] += jnp.sum(value.astype(F32) * upstream, axis=0, keepdims=True)

            forward(0, b, lanes, x.u_all[b, :, lanes], put)
            return carry

        lax.fori_loop(0, n, first_layer, 0, unroll=4)
        if final:
            hear(clips // 2 - 1)
            send_skips()

        def regrid(i, carry):
            x.u2[i, :, lanes] = nn(x.take_second[i], x.y1[:, lanes]).astype(BF16)
            return carry

        lax.fori_loop(0, n, regrid, 0, unroll=4)
        state[:, lanes] = jnp.zeros((state.shape[0], step), F32)

        def second_layer(b, carry):
            forward(1, b, lanes, x.u2[b, :, lanes], None)
            grads(0, b, tile, x.u_all[b, :, lanes], x.dy1[chunk(b), lanes])
            return carry

        lax.fori_loop(0, n, second_layer, 0, unroll=4)
        if final:
            leave(0, range(chips))
            leave_decays(0)

        def second_grads(i, carry):
            b = lax.rem(2 * chip + 2 + i, n)
            grads(1, b, tile, x.u2[b, :, lanes], x.ct_all[chunk(b), lanes])
            return carry

        lax.fori_loop(0, n - 2, second_grads, 0, unroll=2)
        if final:
            leave(1, range(1, chips))
            leave_chip(0)
        lax.fori_loop(n - 2, n, second_grads, 0, unroll=2)
        if final:
            leave_chip(1)
            leave(1, range(1))
            leave_decays(1)

    for tile in range(len(tiles)):
        pass_tile(tile)
    for copy in clip_copies:
        copy.wait()
    x.summed[...] = jnp.sum(x.clips_in[...], axis=0)
    last = []
    for d in range(1, n):
        to = lax.rem(me + d, n)
        copy = copy_to("seq", to, x.summed, x.parts_in.at[me], x.part, d - 1)
        copy.start()
        last.append(copy)
    x.parts_in[me] = x.summed[...]
    own_input = pltpu.make_async_copy(x.du1.at[me], cut(x.dinput, me), x.load.at[0])
    own_input.start()
    for layer in range(2):
        decays_in[layer][me] = x.decays[layer, me]
    for layer, outs in enumerate(((x.dw1, x.dr1), (x.dw2, x.dr2))):
        twin_copy(layer, twin, 0).wait_recv()
        for k, out in enumerate(outs):
            total = x.params[layer, me, k] + x.twins[layer, 0, k]
            if k == 0:
                for copy in chip_copies[layer * (chips - 1) : (layer + 1) * (chips - 1)]:
                    copy.wait_recv()
            for away in range(1, chips):
                total = total + x.chips_in[layer, away, k].astype(F32)
            out[...] = total.astype(BF16)
    for group in arriving:
        for copy in group:
            copy.wait_send()
    for copy in far + near + chip_copies:
        copy.wait_send()
    for layer in range(2):
        for away in range(chips):
            twin_copy(layer, device(away, 1), away).wait_send()
    for d in range(1, n):
        to = lax.rem(me + d, n)
        last += [input_copy(to, tile, d - 1) for tile in range(len(tiles))]
        last += [decay_copy(0, to, d - 1), decay_copy(1, to, d - 1)]
    for copy in last:
        copy.wait()
    for s in range(n):
        for k, out in enumerate((x.dk1, x.dk2)):
            out[:, s * heads : (s + 1) * heads] = x.parts_in[s, k : k + 1, :heads]
    own_input.wait()


def whole(n, clips, size, factor, *args):
    length, width = args[0].shape
    heads = args[3].shape[1]
    count = args[1].shape[1]
    features, half, chips = heads * size, length // 2, n // 2
    vmem = pl.BlockSpec(memory_space=pltpu.VMEM)
    smem = pl.BlockSpec(memory_space=pltpu.SMEM)
    away = pl.BlockSpec(memory_space=pl.ANY)
    param, decay, gain = (length, count), (n, heads, length), (2, features)
    wide, flat, held, square = (n, length, features), (n * length, features), (n, count, features), (n, length, length)
    order, pick, pair = (n, 1, length), (n, length, n * length), (2, length, count)
    outs = (((length, width), BF16),) + ((param, BF16),) * 4 + ((decay, F32),) * 2 + (((1, n * heads), F32),) * 2
    scratch = dict(
        ct_out=((length, width), BF16),
        ct_wide=((length, width), F32),
        u_all=(wide, BF16),
        ct_all=(flat, BF16),
        ct_first=(flat, BF16),
        w_all=((2, n) + param, BF16),
        r_all=((2, n) + param, BF16),
        g_all=((2,) + decay, F32),
        o1_all=(order, jnp.int32),
        o2_all=(order, jnp.int32),
        grown=((2,) + wide, F32),
        shrunk=((2,) + wide, F32),
        sums=((2, n, 8, features), F32),
        fore=((2,) + square, BF16),
        fore_low=((2,) + square, BF16),
        back=((2,) + square, BF16),
        back_low=((2,) + square, BF16),
        take_first=(pick, BF16),
        take_second=(pick, BF16),
        du2=(flat, BF16),
        dy1=(flat, BF16),
        y1=(flat, BF16),
        u2=(wide, BF16),
        du1=(wide, BF16),
        dys=((2,) + wide, BF16),
        ends=((2,) + held, F32),
        ends_a=((2,) + held, BF16),
        ends_z=((2,) + held, BF16),
        inner=((2,) + wide, F32),
        outer=((2,) + wide, F32),
        us=((2, n, 2, length, features), BF16),
        turns=((2, n, 2, half, features), BF16),
        starts_a=((2,) + held, BF16),
        starts_z=((2,) + held, BF16),
        through=((2, n, 1, features), F32),
        kept_heads=((2, n, length, heads), F32),
        kept_scores=((2,) + square, F32),
        kept_reads=((2, n) + param, F32),
        kept_writes=((2, n) + param, F32),
        state=((count, features), F32),
        adjoint=((count, features), F32),
        params=((2, n) + pair, F32),
        twins=((2, chips) + pair, F32),
        chip_sums=((2, chips) + pair, BF16),
        chips_in=((2, chips) + pair, BF16),
        decays=((2,) + decay, F32),
        skips=(gain, F32),
        by_head=((2, length), F32),
        clips_in=((clips, 2, length), F32),
        summed=((2, length), F32),
        parts_in=((n, 2, length), F32),
    )
    sems = dict(
        move=(n - 1, 4 + 2 * max(1, features // (2 * length))),
        near=(n - 1, 4),
        input=(max(1, features // (2 * length)), n - 1),
        decay=(2, n - 1),
        twin=(2, chips),
        chip=(2, chips),
        clip=(clips - 1,),
        part=(n - 1,),
    )
    taken = sum(math.prod(shape) * jnp.dtype(kind).itemsize for shape, kind in scratch.values())
    return pl.pallas_call(
        functools.partial(whole_kernel, n, clips, size, factor, tuple(scratch), tuple(sems)),
        out_shape=tuple(jax.ShapeDtypeStruct(*out) for out in outs),
        in_specs=[away] + [vmem] * 3 + [smem] + [vmem] * 3 + [smem] + [vmem] * 2 + [away],
        out_specs=[away] + [vmem] * 8,
        scratch_shapes=[pltpu.VMEM(*one) for one in scratch.values()]
        + [pltpu.SemaphoreType.DMA(shape) for shape in sems.values() for _ in range(2)]
        + [pltpu.SemaphoreType.DMA((2,)), pltpu.SemaphoreType.REGULAR((clips // 2 - 1,))],
        compiler_params=pltpu.CompilerParams(
            collective_id=0, has_side_effects=True
        ),
        name="whole",
    )(*args)


def gather_kernel(count, *refs):
    sources, results, held, sems = refs[:count], refs[count : 2 * count], refs[2 * count : 3 * count], refs[-2:]
    pieces = []
    for k, source in enumerate(sources):
        step = max(source.shape[0] // 4, 1) if k == 0 else source.shape[0]
        pieces += [(k, pl.ds(at, step)) for at in range(0, source.shape[0], step)]
    loads, stores = [], []
    for at, (k, rows) in enumerate(pieces):
        loads.append(pltpu.make_async_copy(sources[k].at[rows], held[k].at[rows], sems[0].at[at]))
        stores.append(pltpu.make_async_copy(held[k].at[rows], results[k].at[rows], sems[1].at[at]))
        loads[-1].start()
    for load, store in zip(loads, stores):
        load.wait()
        store.start()
    for store in stores:
        store.wait()


def gather(*results):
    away = pl.BlockSpec(memory_space=pl.ANY)
    count = len(results)
    return pl.pallas_call(
        functools.partial(gather_kernel, count),
        out_shape=tuple(jax.ShapeDtypeStruct(one.shape, one.dtype) for one in results),
        in_specs=[away] * count,
        out_specs=[away] * count,
        scratch_shapes=[pltpu.VMEM(one.shape, one.dtype) for one in results]
        + [pltpu.SemaphoreType.DMA((count + 3,))] * 2,
        name="gather",
    )(*results)


def on_device(n, clips, u, w1, r1, g1, k1, w2, r2, g2, k2, o1, o2, ct):
    length, features = u.shape[1:]
    head_count = k1.shape[0]
    size = features // head_count
    heads = head_count // n

    def by_device(g):
        return g.reshape(n, heads, length)

    results = whole(
        n,
        clips,
        size,
        1.0 / math.sqrt(clips * n * length * size),
        u[0],
        w1[0],
        r1[0],
        by_device(g1),
        k1,
        w2[0],
        r2[0],
        by_device(g2),
        k2,
        o1[None],
        o2[None],
        ct[0],
    )
    du, dw1, dr1, dw2, dr2, dg1, dg2, dk1, dk2 = gather(*results)
    return (
        du[None],
        dw1[None],
        dr1[None],
        dg1.reshape(1, head_count, length),
        dk1[0],
        dw2[None],
        dr2[None],
        dg2.reshape(1, head_count, length),
        dk2[0],
    )


def solution(mesh):
    tokens, decay = P("dp", "seq", None), P("dp", None, "seq")
    return jax.shard_map(
        functools.partial(on_device, mesh.shape["seq"], mesh.shape["dp"]),
        mesh=mesh,
        in_specs=(tokens, tokens, tokens, decay, P(), tokens, tokens, decay, P(), P("seq"), P("seq"), tokens),
        out_specs=(tokens, tokens, tokens, decay, P(), tokens, tokens, decay, P()),
        check_vma=False,
    )
```

```python
import functools
import math
import types

import jax
import jax.numpy as jnp
from jax import lax
from jax.experimental import pallas as pl
from jax.experimental.pallas import tpu as pltpu
from jax.sharding import PartitionSpec as P

MESH = pl.DeviceIdType.MESH
HIGHEST = lax.Precision.HIGHEST
F32 = jnp.float32
BF16 = jnp.bfloat16


def nn(a, b, precision=None):
    return lax.dot_general(a, b, (((1,), (0,)), ((), ())), precision=precision, preferred_element_type=F32)


def nt(a, b, precision=None):
    return lax.dot_general(a, b, (((1,), (1,)), ((), ())), precision=precision, preferred_element_type=F32)


def tn(a, b, precision=None):
    return lax.dot_general(a, b, (((0,), (0,)), ((), ())), precision=precision, preferred_element_type=F32)


def iota(shape, dim):
    return lax.broadcasted_iota(jnp.int32, shape, dim)


def two(a):
    high = a.astype(BF16)
    return high, (a - high.astype(F32)).astype(BF16)


def rows_of(*parts):
    return jnp.concatenate(parts, axis=0)


def decay_sums(length):
    half, mid = length // 2, length // 4
    t, s = iota((length + 8, length), 0), iota((length + 8, length), 1)
    first, second = mid, half + mid
    middle = jnp.where(t < half, first, second)
    by_token = (s <= t).astype(F32) - (s < middle).astype(F32)
    k = t - length
    by_chunk = jnp.where(k == 0, (s < first).astype(F32), 0.0)
    by_chunk = jnp.where(k == 1, (s < second).astype(F32), by_chunk)
    by_chunk = jnp.where(k == 2, (s >= first).astype(F32), by_chunk)
    by_chunk = jnp.where(k == 3, (s >= second).astype(F32), by_chunk)
    by_chunk = jnp.where(k == 4, 1.0, by_chunk)
    by_chunk = jnp.where(k == 5, ((s >= first) & (s < second)).astype(F32), by_chunk)
    return jnp.where(k < 0, by_token, by_chunk).astype(BF16)


def factors(log_decay, size):
    heads, length = log_decay.shape
    sums = decay_sums(length)
    wide = [
        jnp.concatenate([jnp.broadcast_to(part[h : h + 1], (size, length)) for h in range(heads)], axis=0).astype(BF16)
        for part in (p.astype(F32) for p in two(log_decay))
    ]
    logs = nt(sums, wide[0]) + nt(sums, wide[1])
    by_token = logs[:length]
    return jnp.exp(by_token), jnp.exp(-by_token), jnp.exp(logs[length:])


def strict_scores(a, b, lower):
    scores = nt(a, b)
    row, col = iota(scores.shape, 0), iota(scores.shape, 1)
    return two(jnp.where(row > col if lower else row < col, scores, 0.0))


def whole_kernel(n, clips, size, factor, held, sems, *refs):
    x = types.SimpleNamespace(**dict(zip(held, refs[21:])))
    x.u, x.w1, x.r1, x.g1, x.k1, x.w2, x.r2, x.g2, x.k2, x.o1, x.o2, x.ct = refs[:12]
    x.dinput, x.dw1, x.dr1, x.dw2, x.dr2, x.decays1_in, x.decays2_in, x.dk1, x.dk2 = refs[12:21]
    x.load, x.rounds = refs[-2:]
    x.__dict__.update(zip(sems, zip(refs[21 + len(held) : -2 : 2], refs[22 + len(held) : -2 : 2])))
    me, clip = lax.axis_index("seq"), lax.axis_index("dp")
    chips = n // 2
    chip, core = lax.div(me, 2), lax.rem(me, 2)
    twin = me + 1 - 2 * core
    heads, length = x.g1.shape[1:]
    features = heads * size
    half = length // 2
    here = pl.ds(pl.multiple_of(me * features, features), features)

    def chunk(b):
        return pl.ds(pl.multiple_of(b * length, length), length)

    def cut(ref, at):
        return ref.at[:, pl.ds(pl.multiple_of(at * features, features), features)]

    barrier = pltpu.get_barrier_semaphore()
    for d in range(1, n):
        pl.semaphore_signal(barrier, inc=1, device_id={"seq": lax.rem(me + d, n)}, device_id_type=MESH)
    lines = ((clip >= 0, clip + 1 - 2 * lax.rem(clip, 2)), (clip >= 2, clip - 2), (clip < clips - 2, clip + 2))
    greetings = sum(jnp.where(there, 1, 0) for there, _ in lines)

    def greet(sem):
        for there, to in lines:

            @pl.when(there)
            def _():
                pl.semaphore_signal(sem, inc=1, device_id={"dp": to}, device_id_type=MESH)

    met = []

    def hear(count):
        for k in range(len(met), count):
            pl.semaphore_wait(x.rounds.at[k], greetings)
            met.append(k)
            if k + 1 < clips // 2 - 1:
                greet(x.rounds.at[k + 1])

    greet(barrier)
    load = pltpu.make_async_copy(x.ct, x.ct_wide, x.load.at[0])
    load.start()
    own_load = pltpu.make_async_copy(cut(x.u, me), x.u_all.at[me], x.load.at[1])
    own_load.start()
    load.wait()
    x.ct_out[...] = x.ct_wide[...].astype(BF16)
    pl.semaphore_wait(barrier, n - 1 + greetings)
    greet(x.rounds.at[0])

    def copy_to(axis, to, src, dst, pair, *at):
        return pltpu.make_async_remote_copy(
            src_ref=src,
            dst_ref=dst,
            send_sem=pair[0].at[at],
            recv_sem=pair[1].at[at],
            device_id={axis: to},
            device_id_type=MESH,
        )

    def device(away, other):
        return 2 * lax.rem(chip + away, chips) + (1 - core if other else core)

    peers = [(away, other) for away in range(1, chips) for other in (0, 1)] + [(0, 1)]
    moves = [
        lambda to: (x.g2.at[to], x.g_all.at[1, me]),
        lambda to: (x.g1.at[to], x.g_all.at[0, me]),
        lambda to: (x.o1, x.o1_all.at[me]),
        lambda to: (x.o2, x.o2_all.at[me]),
    ]
    step = min(2 * length, features)
    tiles = [slice(at, at + step) for at in range(0, features, step)]

    def tile_moves(lanes):
        def at(to):
            return pl.ds(pl.multiple_of(to * features + lanes.start, step), step)

        return [
            lambda to: (x.ct_out.at[:, at(to)], x.ct_all.at[chunk(me), lanes]),
            lambda to: (x.u.at[:, at(to)], x.u_all.at[me, :, lanes]),
        ]

    ct_at = len(moves)
    u_at = ct_at + 1
    for lanes in tiles:
        moves += tile_moves(lanes)
    arriving = [[] for _ in moves]

    def issue(k):
        for away, other in peers:
            to = device(away, other)
            copy = copy_to("seq", to, *moves[k](to), x.move, 2 * away + other - 1, k)
            copy.start()
            arriving[k].append(copy)

    pairs = ((x.w2, x.w_all.at[1]), (x.r2, x.r_all.at[1]), (x.w1, x.w_all.at[0]), (x.r1, x.r_all.at[0]))
    far, near = [], []

    def issue_pair(k):
        src, dst = pairs[k]
        for away in range(1, chips):
            copy = copy_to("seq", device(away, 0), src, dst.at[me], x.near, away - 1, k)
            copy.start()
            far.append(copy)
        copy = copy_to("seq", twin, src, dst.at[me], x.near, chips - 1, k)
        copy.start()
        near.append(copy)

    def wait_for(k):
        for copy in arriving[k]:
            copy.wait_recv()

    issue_pair(0)
    issue_pair(1)
    issue(0)
    issue(1)
    issue_pair(2)
    issue_pair(3)
    for k in range(2, len(moves)):
        issue(k)
    x.g_all[0, me] = x.g1[me]
    x.g_all[1, me] = x.g2[me]
    for src, dst in pairs + ((x.o1, x.o1_all), (x.o2, x.o2_all)):
        dst[me] = src[...]
    x.ct_all[chunk(me)] = x.ct_out[:, here]

    first = me * heads

    def gains(ref):
        channel = iota((1, features), 1) // size
        row = jnp.zeros((1, features), F32)
        for h in range(heads):
            row = jnp.where(channel == h, ref[first + h], row)
        return row

    skips = (gains(x.k1), gains(x.k2))

    def prepare_decays(layer):
        def step(b, carry):
            grown, shrunk, sums = factors(x.g_all[layer, b], size)
            x.grown[layer, b] = grown
            x.shrunk[layer, b] = shrunk
            x.sums[layer, b] = sums
            return carry

        lax.fori_loop(0, n, step, 0, unroll=4)

    def prepare_scores(layer):
        def step(b, carry):
            w, r = x.w_all[layer, b], x.r_all[layer, b]
            x.fore[layer, b], x.fore_low[layer, b] = strict_scores(r, w, True)
            x.back[layer, b], x.back_low[layer, b] = strict_scores(w, r, False)
            return carry

        lax.fori_loop(0, n, step, 0, unroll=4)

    def prepare_order(src, dst, out):
        def step(i, carry):
            cell = jnp.transpose(jnp.broadcast_to(dst[i].astype(F32), (length, length)))
            out[i] = jnp.concatenate([(cell == src[j].astype(F32)).astype(BF16) for j in range(n)], axis=1)
            return carry

        lax.fori_loop(0, n, step, 0, unroll=4)

    wait_for(0)
    hear(1)
    prepare_decays(1)
    wait_for(1)
    prepare_decays(0)
    for copy in far:
        copy.wait_recv()
    for k, (src, dst) in enumerate(pairs):
        for away in range(1, chips):
            block = 2 * lax.rem(chip - away + chips, chips) + core
            copy = copy_to("seq", twin, dst.at[block], dst.at[block], x.near, chips - 1 + away, k)
            copy.start()
            near.append(copy)
    wait_for(2)
    wait_for(3)
    prepare_order(x.o2_all, x.o1_all, x.take_first)
    prepare_order(x.o1_all, x.o2_all, x.take_second)
    for copy in near:
        copy.wait_recv()
    prepare_scores(1)
    prepare_scores(0)
    state, adjoint = x.state, x.adjoint
    adjoint[...] = jnp.zeros_like(adjoint)
    state[...] = jnp.zeros_like(state)

    def own(w, r):
        return jnp.sum(w.astype(F32) * r.astype(F32), axis=1, keepdims=True)

    def back(layer, b, lanes, dy):
        w, r = x.w_all[layer, b], x.r_all[layer, b]
        scores, low = x.back[layer, b], x.back_low[layer, b]
        left_a = jnp.concatenate([w[:half], scores[:half]], axis=1)
        left_z = jnp.concatenate([w[half:], scores[half:]], axis=1)
        wide, sums = dy.astype(F32), x.sums[layer, b, :, lanes]
        scaled = wide * x.grown[layer, b, :, lanes]
        high = scaled.astype(BF16)
        a, z = high[:half], high[half:]
        x.dys[layer, b, :, lanes] = high
        turned = (scaled[half:] * sums[5:6]).astype(BF16)
        end = adjoint[:, lanes]
        carried = rows_of(scaled[:half] * sums[0:1], scaled[half:] * sums[1:2]).astype(BF16)
        adjoint[:, lanes] = end * sums[4:5] + tn(r, carried)
        end_a, end_z = (end * sums[2:3]).astype(BF16), (end * sums[3:4]).astype(BF16)
        x.ends[layer, b, :, lanes] = end
        x.ends_a[layer, b, :, lanes] = end_a
        x.ends_z[layer, b, :, lanes] = end_z
        top = nn(left_a, rows_of(end_a, a, turned)) + nn(low[:half], rows_of(a, turned))
        bottom = nn(left_z, rows_of(end_z, a, z)) + nn(low[half:], high)
        inner = rows_of(top, bottom) * x.shrunk[layer, b, :, lanes]
        x.inner[layer, b, :, lanes] = inner
        return (inner + (skips[layer][:, lanes] + own(w, r)) * wide).astype(BF16)

    lower = iota((length, length), 0) >= iota((length, length), 1)
    since = lower.astype(BF16)
    picks = (iota((features, heads), 0) // size == iota((features, heads), 1)).astype(BF16)

    def forward(layer, b, lanes, u, put):
        w, r = x.w_all[layer, b], x.r_all[layer, b]
        scores, low = x.fore[layer, b], x.fore_low[layer, b]
        left_a = jnp.concatenate([r[:half], scores[:half]], axis=1)
        left_z = jnp.concatenate([r[half:], scores[half:]], axis=1)
        wide, sums = u.astype(F32), x.sums[layer, b, :, lanes]
        scaled = wide * x.shrunk[layer, b, :, lanes]
        high, rest = two(scaled)
        turned, turned_low = two(scaled[:half] * sums[5:6])
        start = state[:, lanes]
        carried, carried_low = two(rows_of(scaled[:half] * sums[2:3], scaled[half:] * sums[3:4]))
        after = start * sums[4:5] + tn(w, carried)
        if put:
            after = after + tn(w, carried_low)
        state[:, lanes] = after
        start_a, start_a_low = two(start * sums[0:1])
        start_z, start_z_low = two(start * sums[1:2])
        other, other_low = rows_of(turned, high[half:]), rows_of(turned_low, rest[half:])
        top = nn(left_a, rows_of(start_a, high))
        bottom = nn(left_z, rows_of(start_z, other))
        if put:
            top = top + nn(low[:half], high) + nn(left_a, rows_of(start_a_low, rest))
            bottom = bottom + nn(low[half:], other) + nn(left_z, rows_of(start_z_low, other_low))
        inner = rows_of(top, bottom) * x.grown[layer, b, :, lanes]
        if put:
            put(wide, (inner + (skips[layer][:, lanes] + own(w, r)) * wide).astype(BF16))
        x.us[layer, b, 0, :, lanes] = high
        if put:
            x.us[layer, b, 1, :, lanes] = rest
            x.turns[layer, b, 1, :, lanes] = turned_low
        x.turns[layer, b, 0, :, lanes] = turned
        x.starts_a[layer, b, :, lanes] = start_a
        x.starts_z[layer, b, :, lanes] = start_z
        x.through[layer, b, :, lanes] = jnp.sum(x.ends[layer, b, :, lanes] * after, axis=0, keepdims=True)
        x.outer[layer, b, :, lanes] = inner

    kept = (x.kept_heads, x.kept_scores, x.kept_reads, x.kept_writes)

    def grads(layer, b, tile, u, dy):
        w, r, lanes = x.w_all[layer, b], x.r_all[layer, b], tiles[tile]
        wide, wide_dy = u.astype(F32), dy.astype(F32)
        terms = wide_dy * x.outer[layer, b, :, lanes] - wide * x.inner[layer, b, :, lanes]
        through = jnp.where(iota((8, step), 0) == 7, x.through[layer, b, :, lanes], 0.0)
        terms, terms_low = two(rows_of(terms[: length - 8], terms[length - 8 :] + through))
        high = x.us[layer, b, 0, :, lanes]
        other = rows_of(x.turns[layer, b, 0, :, lanes], high[half:])
        dys = x.dys[layer, b, :, lanes]
        dy_a, dy_z = dys[:half], dys[half:]
        dscores = rows_of(nt(dy_a, high), nt(dy_z, other))
        if layer == 0:
            rest = x.us[layer, b, 1, :, lanes]
            other_low = rows_of(x.turns[layer, b, 1, :, lanes], rest[half:])
            dscores = dscores + rows_of(nt(dy_a, rest), nt(dy_z, other_low))
        totals = (
            nn(terms, picks[lanes]) + nn(terms_low, picks[lanes]),
            dscores,
            rows_of(nt(dy_a, x.starts_a[layer, b, :, lanes]), nt(dy_z, x.starts_z[layer, b, :, lanes])),
            rows_of(nt(high[:half], x.ends_a[layer, b, :, lanes]), nt(high[half:], x.ends_z[layer, b, :, lanes])),
        )
        totals = (totals[0], jnp.where(lower, totals[1], 0.0)) + totals[2:]
        if tile:
            totals = tuple(part + ref[layer, b] for part, ref in zip(totals, kept))
        if tile < len(tiles) - 1:
            for part, ref in zip(totals, kept):
                ref[layer, b] = part
            return
        by_head, by_head_low = two(totals[0])
        x.decays[layer, b] = tn(by_head, since) + tn(by_head_low, since)
        dscores, dscores_low = two(totals[1])
        x.params[layer, b, 0] = tn(dscores, r) + tn(dscores_low, r) + totals[3]
        x.params[layer, b, 1] = nn(dscores, w) + nn(dscores_low, w) + totals[2]

    decays_in = (x.decays1_in, x.decays2_in)

    def input_copy(to, tile, slot):
        at = pl.ds(pl.multiple_of(me * features + tiles[tile].start, step), step)
        return copy_to("seq", to, x.du1.at[to, :, tiles[tile]], x.dinput.at[:, at], x.input, tile, slot)

    def decay_copy(layer, to, slot):
        return copy_to("seq", to, x.decays.at[layer, to], decays_in[layer].at[me], x.decay, layer, slot)

    def twin_copy(layer, owner, slot):
        return copy_to("seq", twin, x.params.at[layer, owner], x.twins.at[layer, slot], x.twin, layer, slot)

    def leave(layer, ways):
        for away in ways:
            twin_copy(layer, device(away, 1), away).start()

    def leave_decays(layer):
        for d in range(1, n):
            decay_copy(layer, lax.rem(me + d, n), d - 1).start()

    chip_copies = []

    def leave_chip(layer):
        for away in range(1, chips):
            owner = device(away, 0)
            twin_copy(layer, device(away, 1), away).wait_recv()
            total = x.params[layer, owner] + x.twins[layer, away]
            x.chip_sums[layer, away] = total.astype(BF16)
            copy = copy_to(
                "seq", owner, x.chip_sums.at[layer, away], x.chips_in.at[layer, away], x.chip, layer, away
            )
            copy.start()
            chip_copies.append(copy)

    hear(2)
    own_load.wait()
    x.skips[...] = jnp.zeros_like(x.skips)
    clip_copies = []

    def send_skips():
        channel, head = iota((features, length), 0) // size, iota((features, length), 1)
        by_channel, chosen = x.skips[...], (channel == head).astype(BF16)
        high, rest = two(by_channel)
        x.by_head[...] = (nn(high, chosen) + nn(rest, chosen)) * factor
        for d in range(1, clips):
            to = lax.rem(clip + d, clips)
            copy = copy_to("dp", to, x.by_head, x.clips_in.at[clip], x.clip, d - 1)
            copy.start()
            clip_copies.append(copy)
        x.clips_in[clip] = x.by_head[...]

    def pass_tile(tile):
        lanes, final = tiles[tile], tile == len(tiles) - 1

        wait_for(ct_at + 2 * tile)

        def back_second(i, carry):
            b = n - 1 - i
            x.du2[chunk(b), lanes] = back(1, b, lanes, x.ct_all[chunk(b), lanes])
            return carry

        lax.fori_loop(0, n, back_second, 0, unroll=4)

        def regrid_back(i, carry):
            x.dy1[chunk(i), lanes] = nn(x.take_first[i], x.du2[:, lanes]).astype(BF16)
            x.ct_first[chunk(i), lanes] = nn(x.take_first[i], x.ct_all[:, lanes]).astype(BF16)
            return carry

        lax.fori_loop(0, n, regrid_back, 0, unroll=4)
        adjoint[:, lanes] = jnp.zeros((adjoint.shape[0], step), F32)

        def back_first(i, carry):
            b = n - 1 - i
            x.du1[b, :, lanes] = back(0, b, lanes, x.dy1[chunk(b), lanes])
            return carry

        lax.fori_loop(0, n, back_first, 0, unroll=4)
        for d in range(1, n):
            input_copy(lax.rem(me + d, n), tile, d - 1).start()
        wait_for(u_at + 2 * tile)

        def first_layer(b, carry):
            def put(wide, value):
                x.y1[chunk(b), lanes] = value
                x.skips[0:1, lanes] += jnp.sum(wide * x.dy1[chunk(b), lanes].astype(F32), axis=0, keepdims=True)
                upstream = x.ct_first[chunk(b), lanes].astype(F32)
                x.skips[1:2, lanes] += jnp.sum(value.astype(F32) * upstream, axis=0, keepdims=True)

            forward(0, b, lanes, x.u_all[b, :, lanes], put)
            return carry

        lax.fori_loop(0, n, first_layer, 0, unroll=4)
        if final:
            hear(clips // 2 - 1)
            send_skips()

        def regrid(i, carry):
            x.u2[i, :, lanes] = nn(x.take_second[i], x.y1[:, lanes]).astype(BF16)
            return carry

        lax.fori_loop(0, n, regrid, 0, unroll=4)
        state[:, lanes] = jnp.zeros((state.shape[0], step), F32)

        def second_layer(b, carry):
            forward(1, b, lanes, x.u2[b, :, lanes], None)
            grads(0, b, tile, x.u_all[b, :, lanes], x.dy1[chunk(b), lanes])
            return carry

        lax.fori_loop(0, n, second_layer, 0, unroll=4)
        if final:
            leave(0, range(chips))
            leave_decays(0)

        def second_grads(i, carry):
            b = lax.rem(2 * chip + 2 + i, n)
            grads(1, b, tile, x.u2[b, :, lanes], x.ct_all[chunk(b), lanes])
            return carry

        lax.fori_loop(0, n - 2, second_grads, 0, unroll=2)
        if final:
            leave(1, range(1, chips))
            leave_chip(0)
        lax.fori_loop(n - 2, n, second_grads, 0, unroll=2)
        if final:
            leave_chip(1)
            leave(1, range(1))
            leave_decays(1)

    for tile in range(len(tiles)):
        pass_tile(tile)
    for copy in clip_copies:
        copy.wait()
    x.summed[...] = jnp.sum(x.clips_in[...], axis=0)
    last = []
    for d in range(1, n):
        to = lax.rem(me + d, n)
        copy = copy_to("seq", to, x.summed, x.parts_in.at[me], x.part, d - 1)
        copy.start()
        last.append(copy)
    x.parts_in[me] = x.summed[...]
    own_input = pltpu.make_async_copy(x.du1.at[me], cut(x.dinput, me), x.load.at[0])
    own_input.start()
    for layer in range(2):
        decays_in[layer][me] = x.decays[layer, me]
    for layer, outs in enumerate(((x.dw1, x.dr1), (x.dw2, x.dr2))):
        twin_copy(layer, twin, 0).wait_recv()
        for k, out in enumerate(outs):
            total = x.params[layer, me, k] + x.twins[layer, 0, k]
            if k == 0:
                for copy in chip_copies[layer * (chips - 1) : (layer + 1) * (chips - 1)]:
                    copy.wait_recv()
            for away in range(1, chips):
                total = total + x.chips_in[layer, away, k].astype(F32)
            out[...] = total.astype(BF16)
    for group in arriving:
        for copy in group:
            copy.wait_send()
    for copy in far + near + chip_copies:
        copy.wait_send()
    for layer in range(2):
        for away in range(chips):
            twin_copy(layer, device(away, 1), away).wait_send()
    for d in range(1, n):
        to = lax.rem(me + d, n)
        last += [input_copy(to, tile, d - 1) for tile in range(len(tiles))]
        last += [decay_copy(0, to, d - 1), decay_copy(1, to, d - 1)]
    for copy in last:
        copy.wait()
    for s in range(n):
        for k, out in enumerate((x.dk1, x.dk2)):
            out[:, s * heads : (s + 1) * heads] = x.parts_in[s, k : k + 1, :heads]
    own_input.wait()


def whole(n, clips, size, factor, *args):
    length, width = args[0].shape
    heads = args[3].shape[1]
    count = args[1].shape[1]
    features, half, chips = heads * size, length // 2, n // 2
    vmem = pl.BlockSpec(memory_space=pltpu.VMEM)
    smem = pl.BlockSpec(memory_space=pltpu.SMEM)
    away = pl.BlockSpec(memory_space=pl.ANY)
    param, decay, gain = (length, count), (n, heads, length), (2, features)
    wide, flat, held, square = (n, length, features), (n * length, features), (n, count, features), (n, length, length)
    order, pick, pair = (n, 1, length), (n, length, n * length), (2, length, count)
    outs = (((length, width), BF16),) + ((param, BF16),) * 4 + ((decay, F32),) * 2 + (((1, n * heads), F32),) * 2
    scratch = dict(
        ct_out=((length, width), BF16),
        ct_wide=((length, width), F32),
        u_all=(wide, BF16),
        ct_all=(flat, BF16),
        ct_first=(flat, BF16),
        w_all=((2, n) + param, BF16),
        r_all=((2, n) + param, BF16),
        g_all=((2,) + decay, F32),
        o1_all=(order, jnp.int32),
        o2_all=(order, jnp.int32),
        grown=((2,) + wide, F32),
        shrunk=((2,) + wide, F32),
        sums=((2, n, 8, features), F32),
        fore=((2,) + square, BF16),
        fore_low=((2,) + square, BF16),
        back=((2,) + square, BF16),
        back_low=((2,) + square, BF16),
        take_first=(pick, BF16),
        take_second=(pick, BF16),
        du2=(flat, BF16),
        dy1=(flat, BF16),
        y1=(flat, BF16),
        u2=(wide, BF16),
        du1=(wide, BF16),
        dys=((2,) + wide, BF16),
        ends=((2,) + held, F32),
        ends_a=((2,) + held, BF16),
        ends_z=((2,) + held, BF16),
        inner=((2,) + wide, F32),
        outer=((2,) + wide, F32),
        us=((2, n, 2, length, features), BF16),
        turns=((2, n, 2, half, features), BF16),
        starts_a=((2,) + held, BF16),
        starts_z=((2,) + held, BF16),
        through=((2, n, 1, features), F32),
        kept_heads=((2, n, length, heads), F32),
        kept_scores=((2,) + square, F32),
        kept_reads=((2, n) + param, F32),
        kept_writes=((2, n) + param, F32),
        state=((count, features), F32),
        adjoint=((count, features), F32),
        params=((2, n) + pair, F32),
        twins=((2, chips) + pair, F32),
        chip_sums=((2, chips) + pair, BF16),
        chips_in=((2, chips) + pair, BF16),
        decays=((2,) + decay, F32),
        skips=(gain, F32),
        by_head=((2, length), F32),
        clips_in=((clips, 2, length), F32),
        summed=((2, length), F32),
        parts_in=((n, 2, length), F32),
    )
    sems = dict(
        move=(n - 1, 4 + 2 * max(1, features // (2 * length))),
        near=(n - 1, 4),
        input=(max(1, features // (2 * length)), n - 1),
        decay=(2, n - 1),
        twin=(2, chips),
        chip=(2, chips),
        clip=(clips - 1,),
        part=(n - 1,),
    )
    taken = sum(math.prod(shape) * jnp.dtype(kind).itemsize for shape, kind in scratch.values())
    return pl.pallas_call(
        functools.partial(whole_kernel, n, clips, size, factor, tuple(scratch), tuple(sems)),
        out_shape=tuple(jax.ShapeDtypeStruct(*out) for out in outs),
        in_specs=[away] + [vmem] * 3 + [smem] + [vmem] * 3 + [smem] + [vmem] * 2 + [away],
        out_specs=[away] + [vmem] * 8,
        scratch_shapes=[pltpu.VMEM(*one) for one in scratch.values()]
        + [pltpu.SemaphoreType.DMA(shape) for shape in sems.values() for _ in range(2)]
        + [pltpu.SemaphoreType.DMA((2,)), pltpu.SemaphoreType.REGULAR((clips // 2 - 1,))],
        compiler_params=pltpu.CompilerParams(
            collective_id=0, has_side_effects=True
        ),
        name="whole",
    )(*args)


def gather_kernel(count, *refs):
    sources, results, held, sems = refs[:count], refs[count : 2 * count], refs[2 * count : 3 * count], refs[-2:]
    pieces = []
    for k, source in enumerate(sources):
        step = max(source.shape[0] // 4, 1) if k == 0 else source.shape[0]
        pieces += [(k, pl.ds(at, step)) for at in range(0, source.shape[0], step)]
    loads, stores = [], []
    for at, (k, rows) in enumerate(pieces):
        loads.append(pltpu.make_async_copy(sources[k].at[rows], held[k].at[rows], sems[0].at[at]))
        stores.append(pltpu.make_async_copy(held[k].at[rows], results[k].at[rows], sems[1].at[at]))
        loads[-1].start()
    for load, store in zip(loads, stores):
        load.wait()
        store.start()
    for store in stores:
        store.wait()


def gather(*results):
    away = pl.BlockSpec(memory_space=pl.ANY)
    count = len(results)
    return pl.pallas_call(
        functools.partial(gather_kernel, count),
        out_shape=tuple(jax.ShapeDtypeStruct(one.shape, one.dtype) for one in results),
        in_specs=[away] * count,
        out_specs=[away] * count,
        scratch_shapes=[pltpu.VMEM(one.shape, one.dtype) for one in results]
        + [pltpu.SemaphoreType.DMA((count + 3,))] * 2,
        name="gather",
    )(*results)


def on_device(n, clips, u, w1, r1, g1, k1, w2, r2, g2, k2, o1, o2, ct):
    length, features = u.shape[1:]
    head_count = k1.shape[0]
    size = features // head_count
    heads = head_count // n

    def by_device(g):
        return g.reshape(n, heads, length)

    results = whole(
        n,
        clips,
        size,
        1.0 / math.sqrt(clips * n * length * size),
        u[0],
        w1[0],
        r1[0],
        by_device(g1),
        k1,
        w2[0],
        r2[0],
        by_device(g2),
        k2,
        o1[None],
        o2[None],
        ct[0],
    )
    du, dw1, dr1, dw2, dr2, dg1, dg2, dk1, dk2 = gather(*results)
    return (
        du[None],
        dw1[None],
        dr1[None],
        dg1.reshape(1, head_count, length),
        dk1[0],
        dw2[None],
        dr2[None],
        dg2.reshape(1, head_count, length),
        dk2[0],
    )


def solution(mesh):
    tokens, decay = P("dp", "seq", None), P("dp", None, "seq")
    return jax.shard_map(
        functools.partial(on_device, mesh.shape["seq"], mesh.shape["dp"]),
        mesh=mesh,
        in_specs=(tokens, tokens, tokens, decay, P(), tokens, tokens, decay, P(), P("seq"), P("seq"), tokens),
        out_specs=(tokens, tokens, tokens, decay, P(), tokens, tokens, decay, P()),
        check_vma=False,
    )
```
